128 devices in a mesh: chan: 4 (over x), rows: 32 (over z, y, core).
Axes of the slice: x: 4, y: 4, z: 4, core: 2. Of those that a mesh axis runs over, the one named last changes fastest.
Arguments:
- residual: float32 [4, 1024, 16384], P('chan', 'rows'), may hold values from -6 to 6
- psf: float32 [4, 2048, 2048], P('chan', 'rows'), may hold values from -2 to 2
- positions: int32 [32, 2], replicated, may hold values from 0 to 15360, as said below
Outputs:
- residual_out: float32 [4, 1024, 16384], P('chan', 'rows')
- normalized: float32 [1024, 16384], P('rows', 'chan')
The draws below stay inside these ranges and needn't reach their ends.
Inputs may be any that keep to these rules, and one draw needn't show every extreme that they name: positions[k, 0] is a row of the image, 0 to 1023; positions[k, 1] is a column from 1024 to 15360.
All inputs are finite; a program needn't handle non-finite values.
Results may differ from the reference program's by a relative error of at most 0.0001.
Values sent between devices are 32-bit elements; how exact they have to be, the bound alone decides.
A program may use at most 128 MiB of HBM per device.

```python
import jax
import jax.numpy as jnp
from jax import lax

CHANNELS = 4
NCOL = 16384
PATCH = 2048
STEPS = 32
NX = 1024


def draw_positions(key, part):
    half = PATCH // 2
    row_key = jax.random.fold_in(key, 11)
    col_key = jax.random.fold_in(key, 12)
    pick_key = jax.random.fold_in(key, 13)
    rows = jax.random.randint(row_key, (STEPS,), 0, NX)
    cols = jax.random.randint(col_key, (STEPS,), half, NCOL - half + 1)
    picks = jax.random.randint(pick_key, (2,), 0, STEPS)
    low_step = picks[0]
    high_step = (low_step + 1) % STEPS
    rows = rows.at[low_step].set(0)
    rows = rows.at[high_step].set(NX - 1)
    cols = cols.at[picks[1]].set(NCOL - half)
    return jnp.stack([rows, cols], axis=1).astype(jnp.int32)


def block_scale(key, shape, shards, least, largest):
    factor_of, own = 1.0, jax.random.fold_in(key, 6)
    for axis_at, parts in shards:
        draws = jnp.exp(jax.random.uniform(jax.random.fold_in(own, axis_at), (parts,), jnp.float32, least / len(shards), largest / len(shards)))
        factor_of = factor_of * jnp.repeat(draws, shape[axis_at] // parts).reshape([-1 if axis == axis_at else 1 for axis in range(len(shape))])
    return factor_of


def normal_values(key, extent, deviation, reach, pieces=(), dtype=jnp.bfloat16):
    array = deviation * jax.random.normal(key, extent, jnp.float32)
    if pieces:
        array = array * block_scale(key, extent, pieces, -0.22, 0.18)
    return jnp.clip(array, -reach, reach).astype(dtype)


def setup_inputs(seed: int = 0) -> dict:
    key_list = jax.random.split(jax.random.key(seed), 4)
    residual = normal_values(key_list[0], (CHANNELS, NX, NCOL), 1.0, 6.0, ((0, 4), (1, 32)), jnp.float32)
    psf = normal_values(key_list[1], (CHANNELS, PATCH, PATCH), 0.3, 2.0, ((0, 4), (1, 32)), jnp.float32)
    positions = draw_positions(jax.random.fold_in(key_list[3], 71), 0)
    return {"residual": residual, "psf": psf, "positions": positions}


def reference(residual, psf, positions):
    half = PATCH // 2
    padded = jnp.pad(residual, ((0, 0), (half, half), (0, 0)))
    zero = jnp.int32(0)

    def step(k, image):
        row = positions[k, 0].astype(jnp.int32)
        col = positions[k, 1].astype(jnp.int32)
        value = lax.dynamic_slice(image, (zero, row + half, col), (CHANNELS, 1, 1)).reshape(CHANNELS)
        total = jnp.sum(value)
        amp = 0.25 * (value + total / CHANNELS)
        window = lax.dynamic_slice(image, (zero, row, col - half), (CHANNELS, PATCH, PATCH))
        window = window - amp[:, None, None] * psf
        return lax.dynamic_update_slice(image, window, (zero, row, col - half))
    padded = lax.fori_loop(0, STEPS, step, padded)
    image = padded[:, half:half + NX, :]
    summed = lax.optimization_barrier(jnp.sum(image, axis=0))
    mean_square = jnp.mean(summed * summed)
    return (image, summed * lax.rsqrt(mean_square + 1e-06))
```

```python
import functools

import jax
import jax.numpy as jnp
from jax import lax
from jax.experimental import pallas as pl
from jax.experimental.pallas import tpu as pltpu
from jax.sharding import Mesh
from jax.sharding import PartitionSpec as P

STEPS = 32
PAD = 8
LANES = 128
ROWS = ("z", "y", "core")
MESH = pl.DeviceIdType.MESH
F32 = jnp.float32
PIECES = (("z", 1, 0, 3), ("z", -1, 3, 3), ("y", 1, 6, 5), ("y", -1, 11, 5))
HOMES = sorted(((dz, dy) for dz in range(4) for dy in range(4)), key=lambda d: (min(d[0], 4 - d[0]) + min(d[1], 4 - d[1]), d))


def table_kernel(pos, res, psf, own, part, tiles, load_sem, tile_sem):
    unit = 8 * lax.axis_index("z") + 2 * lax.axis_index("y") + lax.axis_index("core")
    slab = res.shape[1]
    rows = own.shape[1] - 2 * PAD
    blocks = own.shape[0]
    half = blocks * LANES // 2
    own_copies = [
        pltpu.make_async_copy(psf.at[0, :, pl.ds(b * LANES, LANES)], own.at[b, pl.ds(PAD, rows)], load_sem.at[b])
        for b in range(blocks)
    ]
    for copy in own_copies:
        copy.start()

    def place(k):
        return pos[k, 0] - unit * slab, pos[k, 1]

    tile_copies = []
    for k in range(STEPS):
        row, col = place(k)
        row = pl.multiple_of(jnp.clip(row, 0, slab - 1) // 8 * 8, 8)
        col = pl.multiple_of(col // LANES * LANES, LANES)
        copy = pltpu.make_async_copy(res.at[0, pl.ds(row, 8), pl.ds(col, LANES)], tiles.at[k], tile_sem.at[k])
        copy.start()
        tile_copies.append(copy)
    for b in range(blocks):
        own[b, :PAD, :] = jnp.zeros((PAD, LANES), F32)
        own[b, PAD + rows :, :] = jnp.zeros((PAD, LANES), F32)
    for copy in own_copies:
        copy.wait()

    wide = lax.broadcasted_iota(jnp.int32, (8, LANES), 1)
    deep = lax.broadcasted_iota(jnp.int32, (8, LANES), 0)

    def placed(tile, base):
        return jnp.where(wide == base + deep, jnp.sum(tile, axis=1, keepdims=True), 0.0)

    def couple(j, total):
        base = LANES // 4 * lax.rem(j, 4)
        for k0 in range(0, STEPS, 8):
            tile = jnp.zeros((8, LANES), F32)
            for s in range(8):
                row = pos[k0 + s, 0] - pos[j, 0] + half - unit * rows
                col = pos[k0 + s, 1] - pos[j, 1] + half
                valid = (row >= 0) & (row < rows) & (col >= 0) & (col < 2 * half)
                col = jnp.clip(col, 0, 2 * half - 1)
                found = own[col // LANES, pl.ds(PAD + jnp.clip(row, 0, rows - 1) - s, 8), :]
                tile = tile + jnp.where((wide == lax.rem(col, LANES)) & (deep == s) & valid, found, 0.0)
            total = total + placed(tile, base + k0)
        return total

    last = STEPS // 4 - 1

    def couple_row(i, carry):
        total = lax.fori_loop(4 * i, 4 * i + 4 - i // last, couple, jnp.zeros((8, LANES), F32))
        part[pl.ds(i, 1), :] = jnp.sum(total, axis=0, keepdims=True)
        return carry

    lax.fori_loop(0, STEPS // 4, couple_row, 0)
    for copy in tile_copies:
        copy.wait()
    total = jnp.zeros((8, LANES), F32)
    for k0 in range(0, STEPS, 8):
        tile = jnp.zeros((8, LANES), F32)
        for s in range(8):
            row, col = place(k0 + s)
            valid = (row >= 0) & (row < slab)
            found = tiles[k0 + s]
            found = jnp.where((wide == lax.rem(col, LANES)) & (deep == lax.rem(row, 8)) & valid, found, 0.0)
            tile = tile + jnp.where(deep == s, jnp.sum(found, axis=0, keepdims=True), 0.0)
        total = total + placed(tile, LANES * 3 // 4 + k0)
    part[last : last + 1, :] = part[last : last + 1, :] + jnp.sum(total, axis=0, keepdims=True)


def peak_table(positions, residual, psf):
    rows, patch = psf.shape[1:]
    sems = pltpu.SemaphoreType.DMA
    return pl.pallas_call(
        table_kernel,
        out_shape=(pltpu.VMEM((patch // LANES, rows + 2 * PAD, LANES), F32), pltpu.VMEM((8, LANES), F32)),
        in_specs=[pl.BlockSpec(memory_space=pltpu.SMEM)] + [pl.BlockSpec(memory_space=pltpu.HBM)] * 2,
        out_specs=(pl.BlockSpec(memory_space=pltpu.VMEM),) * 2,
        scratch_shapes=[pltpu.VMEM((STEPS, 8, LANES), F32), sems((patch // LANES,)), sems((STEPS,))],
        compiler_params=pltpu.CompilerParams(vmem_limit_bytes=8 * 1024 * 1024),
        name="table",
    )(positions, pinned(residual, pltpu.HBM), pinned(psf, pltpu.HBM))


pinned = pltpu.with_memory_space_constraint


def gather_kernel(own, first_part, psf, g, amps, part, got, table, load_sem, send_sem, recv_sem, peer_send, peer_recv, sum_send, sum_recv):
    x, z, y, core = (lax.axis_index(a) for a in ("chan",) + ROWS)
    coord = {"z": z, "y": y, "chan": x, "core": core}
    size = {"z": 4, "y": 4, "chan": 4, "core": 2}
    rows = own.shape[1] - 2 * PAD
    blocks = own.shape[0]

    def device(axis, step):
        return {axis: lax.rem(coord[axis] + step % size[axis], size[axis])}

    barrier = pltpu.get_barrier_semaphore()
    greeted = [("core", 1)] + [(axis, step) for axis in ("y", "z", "chan") for step in (1, 2, 3)]
    for axis, step in greeted:
        pl.semaphore_signal(barrier, inc=1, device_id=device(axis, step), device_id_type=MESH)

    unit = 8 * z + 2 * y + core
    place_copies = [
        pltpu.make_async_copy(psf.at[0, :, pl.ds(b * LANES, LANES)], g.at[b, pl.ds(unit * rows, rows)], load_sem.at[b])
        for b in range(blocks)
    ]
    for copy in place_copies:
        copy.start()
    pl.semaphore_wait(barrier, len(greeted))

    def home(d):
        zh, yh = lax.rem(z + d[0], 4), lax.rem(y + d[1], 4)
        return 4 * zh + yh

    def needed(h, step_z):
        row = lax.rem(z + step_z % 4, 4)
        return jnp.logical_and(h >= 2 * row, h <= 2 * row + 9)

    sends = []

    def forward(d, piece, axis, step, condition):
        first, _, start, count = PIECES[piece]
        rel = list(d)
        rel["zy".index(axis)] = (rel["zy".index(axis)] - step) % 4
        slot = (rel[0] * 4 + rel[1]) * 4 + piece
        dst = g.at[pl.ds(start, count), pl.ds((2 * home(d) + core) * rows, rows)]
        src = own.at[pl.ds(start, count), pl.ds(PAD, rows)] if d == (0, 0) else dst
        copy = pltpu.make_async_remote_copy(src, dst, send_sem.at[len(sends)], recv_sem.at[slot], device_id=device(axis, step), device_id_type=MESH)
        pl.when(condition)(copy.start)
        sends.append((copy, condition))

    def share(d, piece, condition):
        _, _, start, count = PIECES[piece]
        slot = (d[0] * 4 + d[1]) * 4 + piece
        dst = g.at[pl.ds(start, count), pl.ds((2 * home(d) + core) * rows, rows)]
        src = own.at[pl.ds(start, count), pl.ds(PAD, rows)] if d == (0, 0) else dst
        copy = pltpu.make_async_remote_copy(src, dst, peer_send.at[slot], peer_recv.at[slot], device_id=device("core", 1), device_id_type=MESH)
        pl.when(condition)(copy.start)
        return copy

    shares = []

    def arrived(d, piece):
        first, way, start, count = PIECES[piece]
        second = "y" if first == "z" else "z"
        rel = dict(zip("zy", d))
        h = home(d)
        here = needed(h, 0)
        if d != (0, 0):
            slot = (d[0] * 4 + d[1]) * 4 + piece
            dst = g.at[pl.ds(start, count), pl.ds((2 * h + core) * rows, rows)]
            wait = pltpu.make_async_remote_copy(dst, dst, send_sem.at[0], recv_sem.at[slot], device_id=device("core", 1), device_id_type=MESH)
            pl.when(here)(wait.wait_recv)

        def along(axis, step):
            condition = jnp.logical_and(here, needed(h, step)) if axis == "z" else here
            forward(d, piece, axis, step, condition)

        if rel[second] == 0:
            if rel[first] == 0:
                along(first, 1)
                along(first, -1)
            elif rel[first] == -way % 4:
                along(first, way)
            along(second, 1)
            along(second, -1)
        elif rel[second] == -way % 4:
            along(second, way)
        shares.append((share(d, piece, here), here))

    for piece in range(4):
        arrived((0, 0), piece)

    sums = []

    def exchange(axis, value, steps, at):
        copies = []
        for n, step in enumerate(steps):
            copy = pltpu.make_async_remote_copy(
                part.at[value] if value else first_part, got.at[at + n], sum_send.at[at + n], sum_recv.at[at + n], device_id=device(axis, step), device_id_type=MESH
            )
            copies.append(copy)
        return copies

    stages = [("core", (1,), 0), ("y", (1, 2, 3), 1), ("z", (1, 2, 3), 4), ("chan", (3, 2, 1), 7)]
    waves = [[d for d in HOMES if min(d[0], 4 - d[0]) + min(d[1], 4 - d[1]) == n] for n in range(5)]
    todo = [(d, piece) for wave in waves[1:] for d in wave for piece in range(4)]

    pending = []
    taken = 0
    for n, (axis, steps, at) in enumerate(stages):
        copies = exchange(axis, n, steps, at)
        for copy in copies:
            copy.start()
        for d, piece in todo[taken : taken + SHARE_OUT[n]]:
            arrived(d, piece)
        taken += SHARE_OUT[n]
        for copy in copies:
            copy.wait()
        if axis != "chan":
            part[n + 1] = sum((got[at + m] for m in range(len(steps))), part[n] if n else first_part[...])
    tables = [part[3]] + [got[7 + m] for m in range(3)]
    for i in range(STEPS // 4):
        rows_of = jnp.concatenate([t[i : i + 1, :] for t in tables] + [jnp.zeros((4, LANES), F32)], axis=0)
        for m in range(4):
            table[4 * i + m] = rows_of if m == 0 else pltpu.roll(rows_of, LANES - LANES // 4 * m, 1)

    wide = lax.broadcasted_iota(jnp.int32, (8, LANES), 1)

    def solve(j, left):
        value = jnp.sum(jnp.where(wide == j, left, 0.0), axis=1, keepdims=True)
        amp = 0.25 * (value + jnp.sum(value, axis=0, keepdims=True) / 4)
        amps[j] = jnp.broadcast_to(amp[0:1, :], (8, LANES))
        return left - amp * table[j]

    lax.fori_loop(0, STEPS, solve, table[STEPS - 1])

    for d, piece in todo[taken:]:
        arrived(d, piece)
    for copy in place_copies:
        copy.wait()
    for copy, condition in shares:
        pl.when(condition)(copy.wait)
    for copy, condition in sends:
        pl.when(condition)(copy.wait_send)


SHARE_OUT = (0, 8, 8, 8)


def gather(own, part, psf):
    patch = psf.shape[2]
    blocks = patch // LANES
    sems = pltpu.SemaphoreType.DMA
    return pl.pallas_call(
        gather_kernel,
        out_shape=(pltpu.VMEM((blocks, patch, LANES), F32), pltpu.VMEM((STEPS, 8, LANES), F32)),
        in_specs=[pl.BlockSpec(memory_space=pltpu.VMEM)] * 2 + [pl.BlockSpec(memory_space=pltpu.HBM)],
        out_specs=(pl.BlockSpec(memory_space=pltpu.VMEM),) * 2,
        scratch_shapes=[
            pltpu.VMEM((4, 8, LANES), F32),
            pltpu.VMEM((10, 8, LANES), F32),
            pltpu.VMEM((STEPS, 8, LANES), F32),
            sems((blocks,)),
            sems((128,)),
            sems((64,)),
            sems((64,)),
            sems((64,)),
            sems((10,)),
            sems((10,)),
        ],
        compiler_params=pltpu.CompilerParams(collective_id=0, has_side_effects=True, vmem_limit_bytes=8 * 1024 * 1024),
        name="gather",
    )(pinned(own, pltpu.VMEM), pinned(part, pltpu.VMEM), pinned(psf, pltpu.HBM))


def apply_kernel(pos, amps, g, res, out, img, sems):
    load = pltpu.make_async_copy(res.at[0], img, sems.at[0])
    load.start()
    load.wait()
    slab, ncols = img.shape
    blocks = g.shape[0]
    half = blocks * LANES // 2
    first = slab * (8 * lax.axis_index("z") + 2 * lax.axis_index("y") + lax.axis_index("core"))
    lane = lax.broadcasted_iota(jnp.int32, (8, LANES), 1)
    groups = slab // 8

    def step(k, carry):
        start = first - pos[k, 0] + half
        left = pos[k, 1] - half
        block, shift = left // LANES, lax.rem(left, LANES)
        tail = lane >= shift
        amp = amps[k]
        before = [jnp.zeros((8, LANES), F32)] * groups
        terms = []
        for j in range(blocks + 1):
            if j < blocks:
                now = [pltpu.roll(g[j, pl.ds(start + 8 * i, 8), :] * amp, shift, 1) for i in range(groups)]
            else:
                now = [jnp.zeros((8, LANES), F32)] * groups
            terms.append([jnp.where(tail, n, b) for n, b in zip(now, before)])
            before = now
        for j0 in range(0, blocks + 1, 4):
            js = range(j0, min(j0 + 4, blocks + 1))
            cols = [jnp.minimum(block + j, ncols // LANES - 1) if j == blocks else block + j for j in js]
            at = [pl.ds(pl.multiple_of(col * LANES, LANES), LANES) for col in cols]
            old = [[img[8 * i : 8 * i + 8, a] for i in range(groups)] for a in at]
            for j, a, o in zip(js, at, old):
                for i in range(groups):
                    img[8 * i : 8 * i + 8, a] = o[i] - terms[j][i]
        return carry

    lax.fori_loop(0, STEPS, step, 0)
    store = pltpu.make_async_copy(img, out.at[0], sems.at[0])
    store.start()
    store.wait()


def apply_steps(positions, amps, g, residual):
    return pl.pallas_call(
        apply_kernel,
        out_shape=pltpu.HBM(residual.shape, F32),
        in_specs=[pl.BlockSpec(memory_space=pltpu.SMEM)]
        + [pl.BlockSpec(memory_space=pltpu.VMEM)] * 2
        + [pl.BlockSpec(memory_space=pltpu.HBM)],
        out_specs=pl.BlockSpec(memory_space=pltpu.HBM),
        scratch_shapes=[pltpu.VMEM(residual.shape[1:], F32), pltpu.SemaphoreType.DMA((1,))],
        compiler_params=pltpu.CompilerParams(vmem_limit_bytes=8 * 1024 * 1024),
        name="apply",
    )(positions, pinned(amps, pltpu.VMEM), pinned(g, pltpu.VMEM), pinned(residual, pltpu.HBM))


def on_device(residual, psf, positions):
    own, part = peak_table(positions, residual, psf)
    g, amps = gather(own, part, psf)
    image = apply_steps(positions, amps, g, residual)
    count = residual.shape[1] * residual.shape[2] * lax.axis_size(ROWS)
    parts = lax.psum_scatter(image[0], "chan", scatter_dimension=1, tiled=True)
    total = functools.reduce(lax.psum, ("chan",) + ROWS, jnp.sum(parts * parts))
    return image, parts * lax.rsqrt(total / count + 1e-06)


def solution(mesh):
    finer = Mesh(mesh.devices.reshape(mesh.shape["chan"], 4, 4, 2), ("chan",) + ROWS)
    return jax.shard_map(
        on_device,
        mesh=finer,
        in_specs=(P("chan", ROWS, None), P("chan", ROWS, None), P()),
        out_specs=(P("chan", ROWS, None), P(ROWS, "chan")),
        check_vma=False,
    )
```

```python
import functools

import jax
import jax.numpy as jnp
from jax import lax
from jax.experimental import pallas as pl
from jax.experimental.pallas import tpu as pltpu
from jax.sharding import Mesh
from jax.sharding import PartitionSpec as P

STEPS = 32
PAD = 8
LANES = 128
ROWS = ("z", "y", "core")
MESH = pl.DeviceIdType.MESH
F32 = jnp.float32
PIECES = (("z", 1, 0, 3), ("z", -1, 3, 3), ("y", 1, 6, 5), ("y", -1, 11, 5))
HOMES = sorted(((dz, dy) for dz in range(4) for dy in range(4)), key=lambda d: (min(d[0], 4 - d[0]) + min(d[1], 4 - d[1]), d))


def table_kernel(pos, res, psf, own, part, tiles, load_sem, tile_sem):
    unit = 8 * lax.axis_index("z") + 2 * lax.axis_index("y") + lax.axis_index("core")
    slab = res.shape[1]
    rows = own.shape[1] - 2 * PAD
    blocks = own.shape[0]
    half = blocks * LANES // 2
    own_copies = [
        pltpu.make_async_copy(psf.at[0, :, pl.ds(b * LANES, LANES)], own.at[b, pl.ds(PAD, rows)], load_sem.at[b])
        for b in range(blocks)
    ]
    for copy in own_copies:
        copy.start()

    def place(k):
        return pos[0, k] - unit * slab, pos[1, k]

    tile_copies = []
    for k in range(STEPS):
        row, col = place(k)
        row = pl.multiple_of(jnp.clip(row, 0, slab - 1) & ~7, 8)
        col = pl.multiple_of(col & ~127, LANES)
        copy = pltpu.make_async_copy(res.at[0, pl.ds(row, 8), pl.ds(col, LANES)], tiles.at[k], tile_sem.at[k])
        copy.start()
        tile_copies.append(copy)
    for b in range(blocks):
        own[b, :PAD, :] = jnp.zeros((PAD, LANES), F32)
        own[b, PAD + rows :, :] = jnp.zeros((PAD, LANES), F32)
    for copy in own_copies:
        copy.wait()

    wide = lax.broadcasted_iota(jnp.int32, (8, LANES), 1)
    deep = lax.broadcasted_iota(jnp.int32, (8, LANES), 0)

    def placed(tile, base):
        return jnp.where(wide == base + deep, jnp.sum(tile, axis=1, keepdims=True), 0.0)

    def couple(j, carry):
        base_row = half - unit * rows - pos[0, j]
        base_col = half - pos[1, j]
        base = LANES // 4 * (j & 3)
        at = pl.ds(j >> 2, 1)
        for k0 in range(0, STEPS, 8):
            places = [(pos[0, k0 + s] + base_row, pos[1, k0 + s] + base_col) for s in range(8)]
            holds = [(row >= 0) & (row < rows) & (col >= 0) & (col < 2 * half) for row, col in places]

            @pl.when((functools.reduce(jnp.logical_or, holds)) & (k0 + 7 > j))
            def _():
                tile = jnp.zeros((8, LANES), F32)
                for s, ((row, col), held) in enumerate(zip(places, holds)):
                    col = jnp.clip(col, 0, 2 * half - 1)
                    found = own[col >> 7, pl.ds(PAD + jnp.clip(row, 0, rows - 1) - s, 8), :]
                    found = jnp.where((wide == jnp.where(held, col & 127, -1)) & (deep == s), found, 0.0)
                    tile = tile + found
                part[at, :] = part[at, :] + jnp.sum(placed(tile, base + k0), axis=0, keepdims=True)

        return carry

    part[...] = jnp.zeros((8, LANES), F32)
    lax.fori_loop(0, STEPS - 1, couple, 0)
    for copy in tile_copies:
        copy.wait()
    last = STEPS // 4 - 1
    for k0 in range(0, STEPS, 8):
        places = [place(k0 + s) for s in range(8)]
        holds = [(row >= 0) & (row < slab) for row, _ in places]

        @pl.when(functools.reduce(jnp.logical_or, holds))
        def _():
            tile = jnp.zeros((8, LANES), F32)
            for s, ((row, col), held) in enumerate(zip(places, holds)):
                found = jnp.where((wide == (col & 127)) & (deep == jnp.where(held, row & 7, -1)), tiles[k0 + s], 0.0)
                tile = tile + jnp.where(deep == s, jnp.sum(found, axis=0, keepdims=True), 0.0)
            found = jnp.sum(placed(tile, LANES * 3 // 4 + k0), axis=0, keepdims=True)
            part[last : last + 1, :] = part[last : last + 1, :] + found


def peak_table(positions, residual, psf):
    rows, patch = psf.shape[1:]
    sems = pltpu.SemaphoreType.DMA
    return pl.pallas_call(
        table_kernel,
        out_shape=(pltpu.VMEM((patch // LANES, rows + 2 * PAD, LANES), F32), pltpu.VMEM((8, LANES), F32)),
        in_specs=[pl.BlockSpec(memory_space=pltpu.SMEM)] + [pl.BlockSpec(memory_space=pltpu.HBM)] * 2,
        out_specs=(pl.BlockSpec(memory_space=pltpu.VMEM),) * 2,
        scratch_shapes=[pltpu.VMEM((STEPS, 8, LANES), F32), sems((patch // LANES,)), sems((STEPS,))],
        compiler_params=pltpu.CompilerParams(vmem_limit_bytes=8 * 1024 * 1024),
        name="table",
    )(positions, pinned(residual, pltpu.HBM), pinned(psf, pltpu.HBM))


pinned = pltpu.with_memory_space_constraint


def gather_kernel(own, first_part, psf, res, g, amps, img, part, got, table, load_sem, send_sem, recv_sem, peer_send, peer_recv, sum_send, sum_recv):
    x, z, y, core = (lax.axis_index(a) for a in ("chan",) + ROWS)
    coord = {"z": z, "y": y, "chan": x, "core": core}
    size = {"z": 4, "y": 4, "chan": 4, "core": 2}
    rows = own.shape[1] - 2 * PAD
    blocks = own.shape[0]

    def device(axis, step):
        return {axis: lax.rem(coord[axis] + step % size[axis], size[axis])}

    barrier = pltpu.get_barrier_semaphore()
    greeted = [("core", 1)] + [(axis, step) for axis in ("y", "z", "chan") for step in (1, 2, 3)]
    for axis, step in greeted:
        pl.semaphore_signal(barrier, inc=1, device_id=device(axis, step), device_id_type=MESH)

    unit = 8 * z + 2 * y + core
    place_copies = [
        pltpu.make_async_copy(psf.at[0, :, pl.ds(b * LANES, LANES)], g.at[b, pl.ds(unit * rows, rows)], load_sem.at[b])
        for b in range(blocks)
    ]
    place_copies.append(pltpu.make_async_copy(res.at[0], img, load_sem.at[blocks]))
    for copy in place_copies:
        copy.start()
    pl.semaphore_wait(barrier, len(greeted))

    def home(d):
        zh, yh = lax.rem(z + d[0], 4), lax.rem(y + d[1], 4)
        return 4 * zh + yh

    def needed(h, step_z):
        row = lax.rem(z + step_z % 4, 4)
        return jnp.logical_and(h >= 2 * row, h <= 2 * row + 9)

    sends = []

    def forward(d, piece, axis, step, condition):
        first, _, start, count = PIECES[piece]
        rel = list(d)
        rel["zy".index(axis)] = (rel["zy".index(axis)] - step) % 4
        slot = (rel[0] * 4 + rel[1]) * 4 + piece
        dst = g.at[pl.ds(start, count), pl.ds((2 * home(d) + core) * rows, rows)]
        src = own.at[pl.ds(start, count), pl.ds(PAD, rows)] if d == (0, 0) else dst
        copy = pltpu.make_async_remote_copy(src, dst, send_sem.at[len(sends)], recv_sem.at[slot], device_id=device(axis, step), device_id_type=MESH)
        pl.when(condition)(copy.start)
        sends.append((copy, condition))

    def share(d, piece, condition):
        _, _, start, count = PIECES[piece]
        slot = (d[0] * 4 + d[1]) * 4 + piece
        dst = g.at[pl.ds(start, count), pl.ds((2 * home(d) + core) * rows, rows)]
        src = own.at[pl.ds(start, count), pl.ds(PAD, rows)] if d == (0, 0) else dst
        copy = pltpu.make_async_remote_copy(src, dst, peer_send.at[slot], peer_recv.at[slot], device_id=device("core", 1), device_id_type=MESH)
        pl.when(condition)(copy.start)
        return copy

    shares = []

    def arrived(d, piece):
        first, way, start, count = PIECES[piece]
        second = "y" if first == "z" else "z"
        rel = dict(zip("zy", d))
        h = home(d)
        here = needed(h, 0)
        if d != (0, 0):
            slot = (d[0] * 4 + d[1]) * 4 + piece
            dst = g.at[pl.ds(start, count), pl.ds((2 * h + core) * rows, rows)]
            wait = pltpu.make_async_remote_copy(dst, dst, send_sem.at[0], recv_sem.at[slot], device_id=device("core", 1), device_id_type=MESH)
            pl.when(here)(wait.wait_recv)

        def along(axis, step):
            condition = jnp.logical_and(here, needed(h, step)) if axis == "z" else here
            forward(d, piece, axis, step, condition)

        if rel[second] == 0:
            if rel[first] == 0:
                along(first, 1)
                along(first, -1)
            elif rel[first] == -way % 4:
                along(first, way)
            along(second, 1)
            along(second, -1)
        elif rel[second] == -way % 4:
            along(second, way)
        shares.append((share(d, piece, here), here))

    for piece in range(4):
        arrived((0, 0), piece)

    sums = []

    def exchange(axis, value, steps, at):
        copies = []
        for n, step in enumerate(steps):
            copy = pltpu.make_async_remote_copy(
                part.at[value] if value else first_part, got.at[at + n], sum_send.at[at + n], sum_recv.at[at + n], device_id=device(axis, step), device_id_type=MESH
            )
            copies.append(copy)
        return copies

    stages = [("core", (1,), 0), ("y", (1, 2, 3), 1), ("z", (1, 2, 3), 4), ("chan", (3, 2, 1), 7)]
    waves = [[d for d in HOMES if min(d[0], 4 - d[0]) + min(d[1], 4 - d[1]) == n] for n in range(5)]
    todo = [(d, piece) for wave in waves[1:] for d in wave for piece in range(4)]

    pending = []
    taken = 0
    for n, (axis, steps, at) in enumerate(stages):
        copies = exchange(axis, n, steps, at)
        for copy in copies:
            copy.start()
        for d, piece in todo[taken : taken + SHARE_OUT[n]]:
            arrived(d, piece)
        taken += SHARE_OUT[n]
        for copy in copies:
            copy.wait()
        if axis != "chan":
            part[n + 1] = sum((got[at + m] for m in range(len(steps))), part[n] if n else first_part[...])
    tables = [part[3]] + [got[7 + m] for m in range(3)]
    for i in range(STEPS // 4):
        rows_of = jnp.concatenate([t[i : i + 1, :] for t in tables] + [jnp.zeros((4, LANES), F32)], axis=0)
        for m in range(4):
            table[4 * i + m] = rows_of if m == 0 else pltpu.roll(rows_of, LANES - LANES // 4 * m, 1)

    wide = lax.broadcasted_iota(jnp.int32, (8, LANES), 1)

    def solve(j, left):
        value = jnp.sum(jnp.where(wide == j, left, 0.0), axis=1, keepdims=True)
        amp = 0.25 * (value + jnp.sum(value, axis=0, keepdims=True) / 4)
        amps[j] = jnp.broadcast_to(amp[0:1, :], (8, LANES))
        return left - amp * table[j]

    lax.fori_loop(0, STEPS, solve, table[STEPS - 1])

    for d, piece in todo[taken:]:
        arrived(d, piece)
    for copy in place_copies:
        copy.wait()
    for copy, condition in shares:
        pl.when(condition)(copy.wait)
    for copy, condition in sends:
        pl.when(condition)(copy.wait_send)


SHARE_OUT = (0, 8, 8, 8)


def gather(own, part, psf, residual):
    patch = psf.shape[2]
    blocks = patch // LANES
    sems = pltpu.SemaphoreType.DMA
    return pl.pallas_call(
        gather_kernel,
        out_shape=(pltpu.VMEM((blocks, patch, LANES), F32), pltpu.VMEM((STEPS, 8, LANES), F32), pltpu.VMEM(residual.shape[1:], F32)),
        in_specs=[pl.BlockSpec(memory_space=pltpu.VMEM)] * 2 + [pl.BlockSpec(memory_space=pltpu.HBM)] * 2,
        out_specs=(pl.BlockSpec(memory_space=pltpu.VMEM),) * 3,
        scratch_shapes=[
            pltpu.VMEM((4, 8, LANES), F32),
            pltpu.VMEM((10, 8, LANES), F32),
            pltpu.VMEM((STEPS, 8, LANES), F32),
            sems((blocks + 1,)),
            sems((128,)),
            sems((64,)),
            sems((64,)),
            sems((64,)),
            sems((10,)),
            sems((10,)),
        ],
        compiler_params=pltpu.CompilerParams(collective_id=0, has_side_effects=True, vmem_limit_bytes=8 * 1024 * 1024),
        name="gather",
    )(pinned(own, pltpu.VMEM), pinned(part, pltpu.VMEM), pinned(psf, pltpu.HBM), pinned(residual, pltpu.HBM))


def apply_kernel(pos, amps, g, given, img):
    slab, ncols = img.shape
    blocks = g.shape[0]
    half = blocks * LANES // 2
    first = slab * (8 * lax.axis_index("z") + 2 * lax.axis_index("y") + lax.axis_index("core"))
    lane = lax.broadcasted_iota(jnp.int32, (8, LANES), 1)
    groups = slab // 8

    def step(k, carry):
        start = first - pos[0, k] + half
        left = pos[1, k] - half
        block, shift = left >> 7, left & 127
        tail = lane >= shift
        amp = amps[k]
        before = [jnp.zeros((8, LANES), F32)] * groups
        terms = []
        for j in range(blocks + 1):
            if j < blocks:
                now = [pltpu.roll(g[j, pl.ds(start + 8 * i, 8), :] * amp, shift, 1) for i in range(groups)]
            else:
                now = [jnp.zeros((8, LANES), F32)] * groups
            terms.append([jnp.where(tail, n, b) for n, b in zip(now, before)])
            before = now
        for j0 in range(0, blocks + 1, 4):
            js = range(j0, min(j0 + 4, blocks + 1))
            cols = [jnp.minimum(block + j, ncols // LANES - 1) if j == blocks else block + j for j in js]
            at = [pl.ds(pl.multiple_of(col * LANES, LANES), LANES) for col in cols]
            old = [[img[8 * i : 8 * i + 8, a] for i in range(groups)] for a in at]
            for j, a, o in zip(js, at, old):
                for i in range(groups):
                    img[8 * i : 8 * i + 8, a] = o[i] - terms[j][i]
        return carry

    lax.fori_loop(0, STEPS, step, 0)


def apply_steps(positions, amps, g, image):
    return pl.pallas_call(
        apply_kernel,
        out_shape=pltpu.VMEM(image.shape, F32),
        in_specs=[pl.BlockSpec(memory_space=pltpu.SMEM)] + [pl.BlockSpec(memory_space=pltpu.VMEM)] * 3,
        out_specs=pl.BlockSpec(memory_space=pltpu.VMEM),
        input_output_aliases={3: 0},
        compiler_params=pltpu.CompilerParams(vmem_limit_bytes=8 * 1024 * 1024),
        name="apply",
    )(positions, *(pinned(a, pltpu.VMEM) for a in (amps, g, image)))


SPLIT = 4


def reduce_kernel(img, parts, scale, far, near, sums, squares, got, far_send, far_recv, near_send, near_recv, sums_send, sums_recv, sq_send, sq_recv):
    x, z, y, core = (lax.axis_index(a) for a in ("chan",) + ROWS)
    half, width = img.shape[0] // 2, parts.shape[1]
    piece = width // SPLIT

    close = [(dx, dc) for dc in range(2) for dx in range(4) if (dx, dc) != (0, 0)]
    plane = [(dz, dy) for dz in range(4) for dy in range(4) if (dz, dy) != (0, 0)]

    def near_id(dx, dc):
        return {"chan": (x + dx) & 3, "core": (core + dc) & 1}

    def plane_id(dz, dy):
        return {"z": (z + dz) & 3, "y": (y + dy) & 3}

    peers = [near_id(*d) for d in close] + [plane_id(*d) for d in plane]
    barrier = pltpu.get_barrier_semaphore()
    for peer in peers:
        pl.semaphore_signal(barrier, inc=1, device_id=peer, device_id_type=MESH)
    pl.semaphore_wait(barrier, len(peers))

    def cols(chunk, q):
        return pl.ds(pl.multiple_of(((x + chunk) & 3) * width + q * piece, piece), piece)

    def rows(which):
        return pl.ds(which * half, half)

    def send(src, dst, n, q, sems, way):
        copy = pltpu.make_async_remote_copy(
            src, dst.at[n, :, pl.ds(q * piece, piece)], sems[0].at[n * SPLIT + q], sems[1].at[n * SPLIT + q],
            device_id={"chan": (x + way) & 3}, device_id_type=MESH,
        )
        copy.start()
        return copy

    ways = (1, -1)
    fars, nears, lasts = {}, {}, {}
    for q in range(SPLIT):
        for n, way in enumerate(ways):
            fars[n, q] = send(img.at[rows(1 - n), cols(2, q)], far, n, q, (far_send, far_recv), way)
    for q in range(SPLIT):
        for n, way in enumerate(ways):
            nears[n, q] = send(img.at[rows(n), cols(way, q)], near, n, q, (near_send, near_recv), way)
    for q in range(SPLIT):
        for n, way in enumerate(ways):
            fars[n, q].wait_recv()
            at = pl.ds(q * piece, piece)
            far[n, :, at] = far[n, :, at] + img[rows(1 - n), cols(way, q)]
            lasts[n, q] = send(far.at[n, :, at], sums, n, q, (sums_send, sums_recv), way)
    total = jnp.zeros((8, LANES), F32)
    for q in range(SPLIT):
        at = pl.ds(q * piece, piece)
        for n in range(2):
            nears[n, q].wait_recv()
            parts[rows(n), at] = img[rows(n), cols(0, q)] + near[n, :, at]
    for q in range(SPLIT):
        at = pl.ds(q * piece, piece)
        for n in range(2):
            lasts[n, q].wait_recv()
            value = parts[rows(1 - n), at] + sums[n, :, at]
            parts[rows(1 - n), at] = value
            square = value * value
            for i in range(half // 8):
                for t in range(piece // LANES):
                    total = total + square[8 * i : 8 * i + 8, LANES * t : LANES * (t + 1)]

    squares[0] = total
    done = []
    for stage, ids, start in ((0, peers[: len(close)], 0), (1, peers[len(close) :], len(close))):
        copies = [
            pltpu.make_async_remote_copy(squares.at[stage], got.at[start + i], sq_send.at[start + i], sq_recv.at[start + i], device_id=peer, device_id_type=MESH)
            for i, peer in enumerate(ids)
        ]
        for copy in copies:
            copy.start()
        for copy in copies:
            copy.wait_recv()
        done += copies
        squares[stage + 1] = sum((got[start + i] for i in range(len(ids))), squares[stage])
    total = jnp.sum(jnp.sum(squares[2], axis=1, keepdims=True), axis=0, keepdims=True)
    count = img.shape[0] * img.shape[1] * 32
    scale[...] = jnp.broadcast_to(lax.rsqrt(total / count + 1e-06), (8, LANES))
    for copy in list(fars.values()) + list(nears.values()) + list(lasts.values()) + done:
        copy.wait_send()


def reduce_channels(image):
    slab, ncols = image.shape
    width = ncols // 4
    sems = pltpu.SemaphoreType.DMA
    return pl.pallas_call(
        reduce_kernel,
        out_shape=(pltpu.VMEM((slab, width), F32), pltpu.VMEM((8, LANES), F32)),
        in_specs=[pl.BlockSpec(memory_space=pltpu.VMEM)],
        out_specs=(pl.BlockSpec(memory_space=pltpu.VMEM),) * 2,
        scratch_shapes=[pltpu.VMEM((2, slab // 2, width), F32)] * 3
        + [pltpu.VMEM((3, 8, LANES), F32), pltpu.VMEM((22, 8, LANES), F32)]
        + [sems((2 * SPLIT,))] * 6
        + [sems((22,))] * 2,
        compiler_params=pltpu.CompilerParams(collective_id=1, has_side_effects=True, vmem_limit_bytes=8 * 1024 * 1024),
        name="reduce",
    )(pinned(image, pltpu.VMEM))


def write_kernel(img, parts, scale, image_out, normal_out, normal, sems):
    copies = [pltpu.make_async_copy(img, image_out.at[0], sems.at[0])]
    copies[0].start()
    piece = parts.shape[1] // 4
    for q in range(4):
        at = pl.ds(q * piece, piece)
        normal[:, at] = parts[:, at] * scale[0:1, 0:1]
        copies.append(pltpu.make_async_copy(normal.at[:, at], normal_out.at[:, at], sems.at[q + 1]))
        copies[-1].start()
    for copy in copies:
        copy.wait()


def write(image, parts, scale):
    return pl.pallas_call(
        write_kernel,
        out_shape=(pltpu.HBM((1,) + image.shape, F32), pltpu.HBM(parts.shape, F32)),
        in_specs=[pl.BlockSpec(memory_space=pltpu.VMEM)] * 3,
        out_specs=(pl.BlockSpec(memory_space=pltpu.HBM),) * 2,
        scratch_shapes=[pltpu.VMEM(parts.shape, F32), pltpu.SemaphoreType.DMA((5,))],
        compiler_params=pltpu.CompilerParams(vmem_limit_bytes=8 * 1024 * 1024),
        name="write",
    )(*(pinned(a, pltpu.VMEM) for a in (image, parts, scale)))


def on_device(residual, psf, positions):
    positions = positions.T
    own, part = peak_table(positions, residual, psf)
    g, amps, image = gather(own, part, psf, residual)
    image = apply_steps(positions, amps, g, image)
    parts, scale = reduce_channels(image)
    return write(image, parts, scale)


def solution(mesh):
    finer = Mesh(mesh.devices.reshape(mesh.shape["chan"], 4, 4, 2), ("chan",) + ROWS)
    return jax.shard_map(
        on_device,
        mesh=finer,
        in_specs=(P("chan", ROWS, None), P("chan", ROWS, None), P()),
        out_specs=(P("chan", ROWS, None), P(ROWS, "chan")),
        check_vma=False,
    )
```

```python
import functools

import jax
import jax.numpy as jnp
from jax import lax
from jax.experimental import pallas as pl
from jax.experimental.pallas import tpu as pltpu
from jax.sharding import Mesh
from jax.sharding import PartitionSpec as P

STEPS = 32
PAD = 8
LANES = 128
ROWS = ("z", "y", "core")
MESH = pl.DeviceIdType.MESH
F32 = jnp.float32
PIECES = (("z", 1, 0, 4), ("z", -1, 4, 4), ("y", 1, 8, 4), ("y", -1, 12, 4))
ONE, TWO = (1, 3), (2,)
ZY, YZ = (0, 1), (2, 3)


def order():
    def both(firsts, seconds):
        return [
            item
            for f in firsts
            for s in seconds
            for half in range(2)
            for item in (((f, s), ZY[half]), ((s, f), YZ[half]))
        ]

    return [
        both(ONE, (0,)),
        both((0,), ONE),
        both(TWO, (0,)),
        both(ONE, ONE),
        both((0,), TWO),
        both(TWO, ONE),
        both(ONE, TWO) + both(TWO, TWO),
    ]


def table_kernel(pos, res, psf, own, part, tiles, load_sem, tile_sem):
    unit = 8 * lax.axis_index("z") + 2 * lax.axis_index("y") + lax.axis_index("core")
    slab = res.shape[1]
    rows = own.shape[1] - 2 * PAD
    blocks = own.shape[0]
    half = blocks * LANES // 2
    assert (rows, half) == (64, 1024)
    own_copies = [
        pltpu.make_async_copy(psf.at[0, :, pl.ds(b * LANES, LANES)], own.at[b, pl.ds(PAD, rows)], load_sem.at[b])
        for b in range(blocks)
    ]
    for copy in own_copies:
        copy.start()

    def place(k):
        return pos[0, k] - unit * slab, pos[1, k]

    tile_copies = []
    for k in range(STEPS):
        row, col = place(k)
        row = pl.multiple_of(jnp.clip(row, 0, slab - 1) & ~7, 8)
        col = pl.multiple_of(col & ~127, LANES)
        copy = pltpu.make_async_copy(res.at[0, pl.ds(row, 8), pl.ds(col, LANES)], tiles.at[k], tile_sem.at[k])
        copy.start()
        tile_copies.append(copy)
    for b in range(blocks):
        own[b, :PAD, :] = jnp.zeros((PAD, LANES), F32)
        own[b, PAD + rows :, :] = jnp.zeros((PAD, LANES), F32)
    for copy in own_copies:
        copy.wait()

    wide = lax.broadcasted_iota(jnp.int32, (8, LANES), 1)
    deep = lax.broadcasted_iota(jnp.int32, (8, LANES), 0)

    def placed(tile, base):
        return jnp.where(wide == base + deep, jnp.sum(tile, axis=1, keepdims=True), 0.0)

    part[...] = jnp.zeros((8, LANES), F32)
    for k0 in range(0, STEPS, 8):
        peaks = [(pos[0, k0 + s] + half - unit * rows, pos[1, k0 + s] + half) for s in range(8)]

        def couple(j, carry):
            places = [(row - pos[0, j], col - pos[1, j]) for row, col in peaks]
            away = [lax.shift_right_logical(row, 6) | lax.shift_right_logical(col, 11) for row, col in places]

            @pl.when(functools.reduce(jnp.minimum, away) == 0)
            def _():
                tile = jnp.zeros((8, LANES), F32)
                for s, ((row, col), far) in enumerate(zip(places, away)):
                    found = own[(col >> 7) & 15, pl.ds(PAD + (row & 63) - s, 8), :]
                    tile = tile + jnp.where((wide == jnp.where(far == 0, col & 127, -1)) & (deep == s), found, 0.0)
                at = pl.ds(j >> 2, 1)
                part[at, :] = part[at, :] + jnp.sum(placed(tile, LANES // 4 * (j & 3) + k0), axis=0, keepdims=True)

            return carry

        lax.fori_loop(0, min(k0 + 7, STEPS - 1), couple, 0)
    for copy in tile_copies:
        copy.wait()
    last = STEPS // 4 - 1
    for k0 in range(0, STEPS, 8):
        places = [place(k0 + s) for s in range(8)]
        holds = [(row >= 0) & (row < slab) for row, _ in places]

        @pl.when(functools.reduce(jnp.logical_or, holds))
        def _():
            tile = jnp.zeros((8, LANES), F32)
            for s, ((row, col), held) in enumerate(zip(places, holds)):
                found = jnp.where((wide == (col & 127)) & (deep == jnp.where(held, row & 7, -1)), tiles[k0 + s], 0.0)
                tile = tile + jnp.where(deep == s, jnp.sum(found, axis=0, keepdims=True), 0.0)
            found = jnp.sum(placed(tile, LANES * 3 // 4 + k0), axis=0, keepdims=True)
            part[last : last + 1, :] = part[last : last + 1, :] + found


def peak_table(positions, residual, psf):
    rows, patch = psf.shape[1:]
    sems = pltpu.SemaphoreType.DMA
    return pl.pallas_call(
        table_kernel,
        out_shape=(pltpu.VMEM((patch // LANES, rows + 2 * PAD, LANES), F32), pltpu.VMEM((8, LANES), F32)),
        in_specs=[pl.BlockSpec(memory_space=pltpu.SMEM)] + [pl.BlockSpec(memory_space=pltpu.HBM)] * 2,
        out_specs=(pl.BlockSpec(memory_space=pltpu.VMEM),) * 2,
        scratch_shapes=[pltpu.VMEM((STEPS, 8, LANES), F32), sems((patch // LANES,)), sems((STEPS,))],
        compiler_params=pltpu.CompilerParams(vmem_limit_bytes=8 * 1024 * 1024),
        name="table",
    )(positions, pinned(residual, pltpu.HBM), pinned(psf, pltpu.HBM))


pinned = pltpu.with_memory_space_constraint


def gather_kernel(own, first_part, psf, res, g, amps, img, part, got, table, load_sem, send_sem, recv_sem, peer_send, peer_recv, sum_send, sum_recv):
    x, z, y, core = (lax.axis_index(a) for a in ("chan",) + ROWS)
    coord = {"z": z, "y": y, "chan": x, "core": core}
    size = {"z": 4, "y": 4, "chan": 4, "core": 2}
    rows = own.shape[1] - 2 * PAD
    blocks = own.shape[0]

    def device(axis, step):
        return {axis: lax.rem(coord[axis] + step % size[axis], size[axis])}

    barrier = pltpu.get_barrier_semaphore()
    greeted = [("core", 1)] + [(axis, step) for axis in ("y", "z", "chan") for step in (1, 2, 3)]
    for axis, step in greeted:
        pl.semaphore_signal(barrier, inc=1, device_id=device(axis, step), device_id_type=MESH)

    unit = 8 * z + 2 * y + core
    place_copies = [
        pltpu.make_async_copy(psf.at[0, :, pl.ds(b * LANES, LANES)], g.at[b, pl.ds(unit * rows, rows)], load_sem.at[b])
        for b in range(blocks)
    ]
    place_copies.append(pltpu.make_async_copy(res.at[0], img, load_sem.at[blocks]))
    for copy in place_copies:
        copy.start()
    pl.semaphore_wait(barrier, len(greeted))

    def home(d):
        zh, yh = lax.rem(z + d[0], 4), lax.rem(y + d[1], 4)
        return 4 * zh + yh

    def needed(h, step_z):
        row = lax.rem(z + step_z % 4, 4)
        return jnp.logical_and(h >= 2 * row, h <= 2 * row + 9)

    sends = []

    def forward(d, piece, axis, step, condition):
        first, _, start, count = PIECES[piece]
        rel = list(d)
        rel["zy".index(axis)] = (rel["zy".index(axis)] - step) % 4
        slot = (rel[0] * 4 + rel[1]) * 4 + piece
        dst = g.at[pl.ds(start, count), pl.ds((2 * home(d) + core) * rows, rows)]
        src = own.at[pl.ds(start, count), pl.ds(PAD, rows)] if d == (0, 0) else dst
        copy = pltpu.make_async_remote_copy(src, dst, send_sem.at[len(sends)], recv_sem.at[slot], device_id=device(axis, step), device_id_type=MESH)
        pl.when(condition)(copy.start)
        sends.append((copy, condition))

    def share(d, piece, condition):
        _, _, start, count = PIECES[piece]
        slot = (d[0] * 4 + d[1]) * 4 + piece
        dst = g.at[pl.ds(start, count), pl.ds((2 * home(d) + core) * rows, rows)]
        src = own.at[pl.ds(start, count), pl.ds(PAD, rows)] if d == (0, 0) else dst
        copy = pltpu.make_async_remote_copy(src, dst, peer_send.at[slot], peer_recv.at[slot], device_id=device("core", 1), device_id_type=MESH)
        pl.when(condition)(copy.start)
        return copy

    shares = []

    def arrived(d, piece, phase=None):
        first, way, start, count = PIECES[piece]
        second = "y" if first == "z" else "z"
        rel = dict(zip("zy", d))
        h = home(d)
        here = needed(h, 0)
        if d != (0, 0):
            slot = (d[0] * 4 + d[1]) * 4 + piece
            dst = g.at[pl.ds(start, count), pl.ds((2 * h + core) * rows, rows)]
            wait = pltpu.make_async_remote_copy(dst, dst, send_sem.at[0], recv_sem.at[slot], device_id=device("core", 1), device_id_type=MESH)
            pl.when(here)(wait.wait_recv)

        def along(axis, step, also=True):
            condition = jnp.logical_and(jnp.logical_and(here, needed(h, step)), also) if axis == "z" else here
            forward(d, piece, axis, step, condition)

        def relay(axis):
            if axis == "y":
                if rel["y"] == -way % 4:
                    along("y", way)
            elif rel["z"] == 3:
                along("z", 1, lax.rem(z, 4) == 3)
            elif rel["z"] == 1:
                along("z", -1, lax.rem(z, 4) == 0)

        if d == (0, 0):
            for axis in (first, second) if phase is None else ((first,), (second,))[phase]:
                along(axis, 1)
                along(axis, -1)
            if phase == 0:
                return
        elif rel[second] == 0:
            relay(first)
            along(second, 1)
            along(second, -1)
        else:
            relay(second)
        shares.append((share(d, piece, here), here))

    sums = []

    def exchange(axis, value, steps, at):
        copies = []
        for n, step in enumerate(steps):
            copy = pltpu.make_async_remote_copy(
                part.at[value] if value else first_part, got.at[at + n], sum_send.at[at + n], sum_recv.at[at + n], device_id=device(axis, step), device_id_type=MESH
            )
            copies.append(copy)
        return copies

    waves = order()
    stages = [("core", (1,), 0), ("y", (1, 2, 3), 1), ("z", (1, 2, 3), 4), ("chan", (3, 2, 1), 7)]
    after = ([], waves[0], waves[1] + waves[2], waves[3])
    for n, (axis, steps, at) in enumerate(stages):
        copies = exchange(axis, n, steps, at)
        for copy in copies:
            copy.start()
        if n == 0:
            for piece in range(4):
                arrived((0, 0), piece, 0)
        if n == 1:
            for piece in range(4):
                arrived((0, 0), piece, 1)
        for d, piece in after[n]:
            arrived(d, piece)
        for copy in copies:
            copy.wait()
        if axis != "chan":
            part[n + 1] = sum((got[at + m] for m in range(len(steps))), part[n] if n else first_part[...])
    for wave in waves[4:6]:
        for d, piece in wave:
            arrived(d, piece)
    tables = [part[3]] + [got[7 + m] for m in range(3)]
    for i in range(STEPS // 4):
        rows_of = jnp.concatenate([t[i : i + 1, :] for t in tables] + [jnp.zeros((4, LANES), F32)], axis=0)
        for m in range(4):
            table[4 * i + m] = rows_of if m == 0 else pltpu.roll(rows_of, LANES - LANES // 4 * m, 1)

    wide = lax.broadcasted_iota(jnp.int32, (8, LANES), 1)

    def solve(j, left):
        value = jnp.sum(jnp.where(wide == j, left, 0.0), axis=1, keepdims=True)
        amp = 0.25 * (value + jnp.sum(value, axis=0, keepdims=True) / 4)
        amps[j] = jnp.broadcast_to(amp[0:1, :], (8, LANES))
        return left - amp * table[j]

    lax.fori_loop(0, STEPS, solve, table[STEPS - 1])

    for d, piece in waves[6]:
        arrived(d, piece)
    for copy in place_copies:
        copy.wait()
    for copy, condition in shares:
        pl.when(condition)(copy.wait)
    for copy, condition in sends:
        pl.when(condition)(copy.wait_send)


def gather(own, part, psf, residual):
    patch = psf.shape[2]
    blocks = patch // LANES
    sems = pltpu.SemaphoreType.DMA
    return pl.pallas_call(
        gather_kernel,
        out_shape=(pltpu.VMEM((blocks, patch, LANES), F32), pltpu.VMEM((STEPS, 8, LANES), F32), pltpu.VMEM(residual.shape[1:], F32)),
        in_specs=[pl.BlockSpec(memory_space=pltpu.VMEM)] * 2 + [pl.BlockSpec(memory_space=pltpu.HBM)] * 2,
        out_specs=(pl.BlockSpec(memory_space=pltpu.VMEM),) * 3,
        scratch_shapes=[
            pltpu.VMEM((4, 8, LANES), F32),
            pltpu.VMEM((10, 8, LANES), F32),
            pltpu.VMEM((STEPS, 8, LANES), F32),
            sems((blocks + 1,)),
            sems((128,)),
            sems((64,)),
            sems((64,)),
            sems((64,)),
            sems((10,)),
            sems((10,)),
        ],
        compiler_params=pltpu.CompilerParams(collective_id=0, has_side_effects=True, vmem_limit_bytes=8 * 1024 * 1024),
        name="gather",
    )(pinned(own, pltpu.VMEM), pinned(part, pltpu.VMEM), pinned(psf, pltpu.HBM), pinned(residual, pltpu.HBM))


def apply_kernel(pos, amps, g, given, img):
    slab, ncols = img.shape
    blocks = g.shape[0]
    half = blocks * LANES // 2
    first = slab * (8 * lax.axis_index("z") + 2 * lax.axis_index("y") + lax.axis_index("core"))
    lane = lax.broadcasted_iota(jnp.int32, (8, LANES), 1)
    groups = slab // 8

    def step(k, carry):
        start = first - pos[0, k] + half
        left = pos[1, k] - half
        block, shift = left >> 7, left & 127
        tail = lane >= shift
        amp = amps[k]
        before = [jnp.zeros((8, LANES), F32)] * groups
        terms = []
        for j in range(blocks + 1):
            if j < blocks:
                now = [pltpu.roll(g[j, pl.ds(start + 8 * i, 8), :] * amp, shift, 1) for i in range(groups)]
            else:
                now = [jnp.zeros((8, LANES), F32)] * groups
            terms.append([jnp.where(tail, n, b) for n, b in zip(now, before)])
            before = now
        for j0 in range(0, blocks + 1, 4):
            js = range(j0, min(j0 + 4, blocks + 1))
            cols = [jnp.minimum(block + j, ncols // LANES - 1) if j == blocks else block + j for j in js]
            at = [pl.ds(pl.multiple_of(col * LANES, LANES), LANES) for col in cols]
            old = [[img[8 * i : 8 * i + 8, a] for i in range(groups)] for a in at]
            for j, a, o in zip(js, at, old):
                for i in range(groups):
                    img[8 * i : 8 * i + 8, a] = o[i] - terms[j][i]
        return carry

    lax.fori_loop(0, STEPS, step, 0)


def apply_steps(positions, amps, g, image):
    return pl.pallas_call(
        apply_kernel,
        out_shape=pltpu.VMEM(image.shape, F32),
        in_specs=[pl.BlockSpec(memory_space=pltpu.SMEM)] + [pl.BlockSpec(memory_space=pltpu.VMEM)] * 3,
        out_specs=pl.BlockSpec(memory_space=pltpu.VMEM),
        input_output_aliases={3: 0},
        compiler_params=pltpu.CompilerParams(vmem_limit_bytes=8 * 1024 * 1024),
        name="apply",
    )(positions, *(pinned(a, pltpu.VMEM) for a in (amps, g, image)))


SPLIT = 4


def reduce_kernel(img, parts, scale, far, near, sums, squares, got, far_send, far_recv, near_send, near_recv, sums_send, sums_recv, sq_send, sq_recv):
    x, z, y, core = (lax.axis_index(a) for a in ("chan",) + ROWS)
    half, width = img.shape[0] // 2, parts.shape[1]
    piece = width // SPLIT

    close = [(dx, dc) for dc in range(2) for dx in range(4) if (dx, dc) != (0, 0)]
    plane = [(dz, dy) for dz in range(4) for dy in range(4) if (dz, dy) != (0, 0)]

    def near_id(dx, dc):
        return {"chan": (x + dx) & 3, "core": (core + dc) & 1}

    def plane_id(dz, dy):
        return {"z": (z + dz) & 3, "y": (y + dy) & 3}

    peers = [near_id(*d) for d in close] + [plane_id(*d) for d in plane]
    barrier = pltpu.get_barrier_semaphore()
    for peer in peers:
        pl.semaphore_signal(barrier, inc=1, device_id=peer, device_id_type=MESH)
    pl.semaphore_wait(barrier, len(peers))

    def cols(chunk, q):
        return pl.ds(pl.multiple_of(((x + chunk) & 3) * width + q * piece, piece), piece)

    def rows(which):
        return pl.ds(which * half, half)

    def send(src, dst, n, q, sems, way):
        copy = pltpu.make_async_remote_copy(
            src, dst.at[n, :, pl.ds(q * piece, piece)], sems[0].at[n * SPLIT + q], sems[1].at[n * SPLIT + q],
            device_id={"chan": (x + way) & 3}, device_id_type=MESH,
        )
        copy.start()
        return copy

    ways = (1, -1)
    fars, nears, lasts = {}, {}, {}
    for q in range(SPLIT):
        for n, way in enumerate(ways):
            fars[n, q] = send(img.at[rows(1 - n), cols(2, q)], far, n, q, (far_send, far_recv), way)
    for q in range(SPLIT):
        for n, way in enumerate(ways):
            nears[n, q] = send(img.at[rows(n), cols(way, q)], near, n, q, (near_send, near_recv), way)
    for q in range(SPLIT):
        for n, way in enumerate(ways):
            fars[n, q].wait_recv()
            at = pl.ds(q * piece, piece)
            far[n, :, at] = far[n, :, at] + img[rows(1 - n), cols(way, q)]
            lasts[n, q] = send(far.at[n, :, at], sums, n, q, (sums_send, sums_recv), way)
    total = jnp.zeros((8, LANES), F32)
    for q in range(SPLIT):
        at = pl.ds(q * piece, piece)
        for n in range(2):
            nears[n, q].wait_recv()
            parts[rows(n), at] = img[rows(n), cols(0, q)] + near[n, :, at]
    for q in range(SPLIT):
        at = pl.ds(q * piece, piece)
        for n in range(2):
            lasts[n, q].wait_recv()
            value = parts[rows(1 - n), at] + sums[n, :, at]
            parts[rows(1 - n), at] = value
            square = value * value
            for i in range(half // 8):
                for t in range(piece // LANES):
                    total = total + square[8 * i : 8 * i + 8, LANES * t : LANES * (t + 1)]

    squares[0] = total
    done = []
    for stage, ids, start in ((0, peers[: len(close)], 0), (1, peers[len(close) :], len(close))):
        copies = [
            pltpu.make_async_remote_copy(squares.at[stage], got.at[start + i], sq_send.at[start + i], sq_recv.at[start + i], device_id=peer, device_id_type=MESH)
            for i, peer in enumerate(ids)
        ]
        for copy in copies:
            copy.start()
        for copy in copies:
            copy.wait_recv()
        done += copies
        squares[stage + 1] = sum((got[start + i] for i in range(len(ids))), squares[stage])
    total = jnp.sum(jnp.sum(squares[2], axis=1, keepdims=True), axis=0, keepdims=True)
    count = img.shape[0] * img.shape[1] * 32
    scale[...] = jnp.broadcast_to(lax.rsqrt(total / count + 1e-06), (8, LANES))
    for copy in list(fars.values()) + list(nears.values()) + list(lasts.values()) + done:
        copy.wait_send()


def reduce_channels(image):
    slab, ncols = image.shape
    width = ncols // 4
    sems = pltpu.SemaphoreType.DMA
    return pl.pallas_call(
        reduce_kernel,
        out_shape=(pltpu.VMEM((slab, width), F32), pltpu.VMEM((8, LANES), F32)),
        in_specs=[pl.BlockSpec(memory_space=pltpu.VMEM)],
        out_specs=(pl.BlockSpec(memory_space=pltpu.VMEM),) * 2,
        scratch_shapes=[pltpu.VMEM((2, slab // 2, width), F32)] * 3
        + [pltpu.VMEM((3, 8, LANES), F32), pltpu.VMEM((22, 8, LANES), F32)]
        + [sems((2 * SPLIT,))] * 6
        + [sems((22,))] * 2,
        compiler_params=pltpu.CompilerParams(collective_id=1, has_side_effects=True, vmem_limit_bytes=8 * 1024 * 1024),
        name="reduce",
    )(pinned(image, pltpu.VMEM))


def write_kernel(img, parts, scale, image_out, normal_out, normal, sems):
    copies = [pltpu.make_async_copy(img, image_out.at[0], sems.at[0])]
    copies[0].start()
    piece = parts.shape[1] // 4
    for q in range(4):
        at = pl.ds(q * piece, piece)
        normal[:, at] = parts[:, at] * scale[0:1, 0:1]
        copies.append(pltpu.make_async_copy(normal.at[:, at], normal_out.at[:, at], sems.at[q + 1]))
        copies[-1].start()
    for copy in copies:
        copy.wait()


def write(image, parts, scale):
    return pl.pallas_call(
        write_kernel,
        out_shape=(pltpu.HBM((1,) + image.shape, F32), pltpu.HBM(parts.shape, F32)),
        in_specs=[pl.BlockSpec(memory_space=pltpu.VMEM)] * 3,
        out_specs=(pl.BlockSpec(memory_space=pltpu.HBM),) * 2,
        scratch_shapes=[pltpu.VMEM(parts.shape, F32), pltpu.SemaphoreType.DMA((5,))],
        compiler_params=pltpu.CompilerParams(vmem_limit_bytes=8 * 1024 * 1024),
        name="write",
    )(*(pinned(a, pltpu.VMEM) for a in (image, parts, scale)))


def on_device(residual, psf, positions):
    positions = positions.T
    own, part = peak_table(positions, residual, psf)
    g, amps, image = gather(own, part, psf, residual)
    image = apply_steps(positions, amps, g, image)
    parts, scale = reduce_channels(image)
    return write(image, parts, scale)


def solution(mesh):
    finer = Mesh(mesh.devices.reshape(mesh.shape["chan"], 4, 4, 2), ("chan",) + ROWS)
    return jax.shard_map(
        on_device,
        mesh=finer,
        in_specs=(P("chan", ROWS, None), P("chan", ROWS, None), P()),
        out_specs=(P("chan", ROWS, None), P(ROWS, "chan")),
        check_vma=False,
    )
```

```python
import functools

import jax
import jax.numpy as jnp
from jax import lax
from jax.experimental import pallas as pl
from jax.experimental.pallas import tpu as pltpu
from jax.sharding import Mesh
from jax.sharding import PartitionSpec as P

STEPS = 32
PAD = 8
LANES = 128
ROWS = ("z", "y", "core")
MESH = pl.DeviceIdType.MESH
F32 = jnp.float32
PIECES = 4
PROGRAM = (
    (65, 265, 269, 268, 193, 194, 73, 273, 277, 196, 209, 210, 529, 137, 473, 533, 138, 475, 476, 457, 513, 321, 281, 141, 459, 276, 201, 202, 521, 345, 337, 525, 460, 217, 218, 537, 385, 449, 285, 387, 212, 129, 130, 451, 81, 393, 541, 284, 145, 146, 325, 395, 89, 465, 349, 467, 153, 154, 409, 329, 257, 341, 401, 403, 0, 0, 0, 0, 0, 0),
    (36, 44, 52, 60, 97, 289, 101, 225, 226, 228, 121, 305, 293, 233, 308, 105, 481, 125, 483, 241, 242, 236, 113, 313, 309, 169, 170, 484, 441, 377, 317, 443, 425, 427, 316, 489, 161, 297, 381, 433, 435, 497, 292, 361, 353, 249, 505, 177, 369, 185, 417, 0, 0, 0, 0, 0, 0, 0, 0, 0, 0, 0, 0, 0, 0, 0, 0, 0, 0, 0),
    (69, 68, 77, 76, 137, 321, 141, 84, 129, 345, 325, 92, 265, 145, 329, 349, 324, 193, 194, 217, 385, 389, 348, 218, 473, 475, 529, 153, 337, 85, 332, 273, 521, 524, 201, 449, 451, 93, 340, 457, 537, 276, 393, 257, 459, 333, 209, 513, 401, 409, 281, 465, 0, 0, 0, 0, 0, 0, 0, 0, 0, 0, 0, 0, 0, 0, 0, 0, 0, 0),
    (101, 108, 125, 116, 33, 161, 361, 41, 162, 109, 100, 49, 177, 353, 178, 57, 117, 124, 185, 441, 186, 443, 225, 445, 444, 226, 425, 417, 427, 305, 165, 308, 419, 545, 169, 553, 170, 233, 365, 555, 234, 689, 241, 505, 690, 507, 481, 181, 242, 561, 433, 369, 483, 313, 314, 569, 249, 377, 435, 250, 289, 497, 489, 297, 491, 0, 0, 0, 0, 0),
    (141, 132, 133, 148, 65, 201, 393, 202, 149, 156, 73, 217, 385, 218, 221, 396, 81, 209, 449, 210, 451, 157, 388, 89, 473, 465, 475, 474, 585, 205, 588, 601, 321, 193, 401, 467, 602, 577, 397, 580, 593, 457, 409, 345, 194, 459, 405, 329, 265, 521, 266, 523, 257, 337, 513, 273, 529, 281, 537, 0, 0, 0, 0, 0, 0, 0, 0, 0, 0, 0),
    (165, 172, 181, 188, 105, 241, 433, 242, 189, 436, 113, 249, 425, 250, 429, 164, 97, 489, 497, 491, 173, 180, 121, 225, 417, 499, 226, 245, 108, 441, 233, 361, 234, 437, 116, 481, 369, 305, 483, 545, 253, 420, 505, 364, 289, 353, 507, 561, 493, 372, 377, 297, 553, 313, 569, 0, 0, 0, 0, 0, 0, 0, 0, 0, 0, 0, 0, 0, 0, 0),
    (196, 205, 212, 221, 129, 457, 460, 213, 145, 473, 204, 477, 265, 266, 153, 401, 220, 197, 273, 393, 257, 132, 461, 529, 531, 530, 385, 449, 148, 269, 137, 513, 514, 585, 465, 587, 156, 261, 521, 601, 523, 522, 577, 409, 602, 404, 579, 281, 285, 578, 329, 537, 539, 593, 321, 345, 337, 0, 0, 0, 0, 0, 0, 0, 0, 0, 0, 0, 0, 0),
    (228, 245, 234, 250, 236, 253, 226, 242, 169, 489, 491, 244, 493, 185, 497, 499, 172, 229, 97, 433, 425, 434, 428, 237, 289, 161, 481, 483, 561, 562, 436, 485, 121, 177, 553, 555, 252, 293, 505, 305, 105, 297, 188, 313, 617, 113, 633, 635, 625, 417, 377, 569, 441, 361, 353, 369, 545, 609, 0, 0, 0, 0, 0, 0, 0, 0, 0, 0, 0, 0),
    (267, 261, 260, 258, 275, 277, 284, 266, 337, 537, 473, 475, 285, 540, 274, 329, 529, 449, 283, 333, 268, 282, 193, 393, 513, 465, 209, 339, 341, 276, 338, 321, 521, 457, 451, 541, 476, 330, 137, 577, 585, 385, 395, 532, 450, 201, 601, 217, 467, 460, 657, 409, 345, 129, 259, 401, 665, 641, 593, 145, 649, 153, 0, 0, 0, 0, 0, 0, 0, 0),
    (291, 301, 300, 290, 307, 317, 308, 314, 353, 553, 481, 483, 557, 556, 298, 377, 569, 497, 315, 357, 572, 306, 225, 633, 545, 489, 379, 637, 500, 354, 361, 561, 417, 299, 293, 292, 418, 241, 441, 369, 505, 355, 309, 484, 498, 609, 233, 169, 365, 617, 433, 371, 492, 442, 381, 425, 434, 613, 161, 177, 249, 625, 185, 0, 0, 0, 0, 0, 0, 0),
    (341, 323, 348, 322, 346, 333, 324, 347, 257, 393, 585, 394, 397, 332, 331, 281, 385, 577, 330, 325, 340, 387, 537, 401, 593, 402, 581, 588, 339, 265, 449, 601, 338, 260, 451, 273, 409, 521, 413, 193, 284, 259, 217, 473, 665, 513, 540, 411, 465, 529, 641, 201, 657, 457, 649, 209, 0, 0, 0, 0, 0, 0, 0, 0, 0, 0, 0, 0, 0, 0),
    (370, 357, 364, 363, 378, 381, 372, 355, 297, 441, 633, 362, 637, 356, 443, 305, 417, 609, 161, 354, 365, 380, 419, 553, 433, 617, 177, 298, 445, 636, 555, 569, 505, 625, 185, 442, 613, 612, 507, 437, 497, 425, 673, 225, 306, 620, 371, 165, 434, 289, 697, 561, 169, 572, 379, 181, 506, 233, 629, 498, 481, 681, 689, 299, 189, 241, 489, 545, 313, 249),
    (410, 397, 404, 395, 388, 389, 387, 386, 345, 449, 665, 396, 405, 451, 394, 321, 465, 641, 412, 453, 467, 402, 201, 329, 457, 657, 348, 413, 403, 346, 721, 217, 337, 705, 209, 649, 668, 669, 411, 330, 644, 585, 729, 713, 469, 458, 324, 473, 205, 660, 257, 273, 593, 338, 661, 724, 577, 601, 213, 588, 281, 513, 193, 521, 537, 529, 265, 0, 0, 0),
    (428, 445, 435, 434, 420, 421, 427, 418, 361, 497, 697, 444, 437, 499, 426, 369, 505, 689, 700, 509, 419, 442, 241, 353, 481, 681, 692, 429, 363, 482, 249, 377, 297, 701, 371, 362, 561, 633, 313, 507, 354, 225, 625, 355, 609, 489, 378, 379, 673, 233, 299, 617, 553, 315, 545, 569, 289, 305, 0, 0, 0, 0, 0, 0, 0, 0, 0, 0, 0, 0),
    (453, 476, 459, 466, 469, 475, 452, 458, 401, 705, 257, 461, 403, 468, 474, 385, 729, 273, 709, 259, 460, 450, 393, 713, 281, 733, 451, 388, 402, 409, 649, 329, 265, 277, 467, 386, 345, 348, 337, 411, 394, 665, 529, 641, 668, 537, 331, 321, 644, 513, 657, 721, 593, 521, 585, 601, 577, 0, 0, 0, 0, 0, 0, 0, 0, 0, 0, 0, 0, 0),
    (501, 491, 484, 506, 509, 499, 500, 490, 233, 425, 737, 249, 297, 485, 427, 492, 482, 225, 417, 745, 241, 313, 301, 483, 420, 498, 441, 673, 553, 317, 555, 508, 426, 697, 753, 353, 493, 299, 236, 418, 433, 545, 428, 689, 761, 633, 677, 635, 442, 561, 681, 252, 557, 569, 289, 443, 354, 549, 617, 305, 293, 361, 362, 625, 355, 309, 377, 369, 609, 0),
    (524, 530, 539, 533, 531, 517, 514, 516, 793, 257, 585, 785, 721, 515, 525, 522, 540, 769, 265, 777, 705, 523, 541, 538, 796, 321, 273, 465, 587, 797, 586, 724, 345, 281, 601, 657, 589, 722, 532, 603, 641, 337, 409, 789, 410, 468, 659, 577, 393, 329, 457, 460, 401, 403, 473, 449, 665, 593, 595, 649, 385, 651, 713, 729, 0, 0, 0, 0, 0, 0),
    (555, 565, 546, 556, 571, 573, 570, 564, 289, 625, 745, 547, 549, 746, 548, 633, 313, 753, 609, 563, 629, 754, 572, 297, 761, 369, 557, 554, 292, 371, 305, 737, 617, 373, 562, 748, 619, 353, 505, 377, 637, 626, 316, 489, 417, 673, 361, 613, 418, 756, 481, 381, 634, 497, 681, 762, 441, 433, 425, 689, 697, 0, 0, 0, 0, 0, 0, 0, 0, 0),
    (602, 588, 587, 589, 579, 596, 578, 321, 521, 657, 325, 595, 580, 594, 345, 513, 641, 349, 603, 516, 522, 769, 393, 537, 649, 645, 523, 524, 538, 777, 329, 793, 665, 397, 515, 324, 658, 586, 401, 721, 713, 405, 643, 540, 650, 385, 785, 666, 669, 337, 529, 409, 651, 796, 722, 389, 714, 465, 705, 457, 729, 473, 449, 0, 0, 0, 0, 0, 0, 0),
    (635, 620, 610, 629, 611, 612, 626, 637, 613, 369, 553, 673, 619, 556, 634, 373, 377, 561, 681, 627, 628, 562, 809, 621, 361, 545, 761, 675, 636, 762, 825, 381, 353, 569, 689, 563, 372, 365, 297, 289, 737, 683, 828, 801, 441, 745, 697, 547, 305, 817, 481, 313, 433, 425, 505, 489, 753, 497, 417, 0, 0, 0, 0, 0, 0, 0, 0, 0, 0, 0),
    (660, 667, 642, 661, 650, 652, 643, 645, 409, 585, 713, 586, 412, 659, 653, 385, 593, 721, 857, 594, 668, 723, 669, 651, 393, 577, 705, 833, 666, 644, 717, 715, 401, 513, 729, 514, 596, 389, 601, 595, 413, 345, 521, 529, 714, 580, 579, 709, 836, 515, 329, 321, 465, 777, 706, 523, 733, 841, 844, 531, 457, 537, 473, 793, 449, 337, 785, 769, 849, 0),
    (690, 676, 699, 677, 698, 684, 691, 685, 433, 617, 761, 674, 620, 683, 765, 417, 609, 737, 682, 692, 693, 425, 553, 561, 563, 618, 700, 741, 441, 625, 569, 627, 554, 436, 809, 481, 633, 489, 485, 801, 570, 361, 369, 745, 493, 817, 610, 353, 825, 753, 634, 497, 505, 377, 545, 0, 0, 0, 0, 0, 0, 0, 0, 0, 0, 0, 0, 0, 0, 0),
    (717, 724, 730, 707, 706, 708, 725, 731, 465, 657, 529, 714, 468, 709, 715, 457, 649, 513, 722, 660, 733, 651, 777, 473, 409, 521, 658, 412, 533, 449, 665, 537, 666, 460, 469, 857, 401, 641, 793, 642, 652, 477, 849, 385, 593, 595, 585, 732, 577, 601, 393, 833, 785, 769, 841, 0, 0, 0, 0, 0, 0, 0, 0, 0, 0, 0, 0, 0, 0, 0),
    (738, 748, 765, 739, 746, 756, 741, 747, 505, 673, 561, 562, 764, 565, 675, 489, 681, 569, 506, 740, 573, 755, 801, 481, 617, 545, 817, 618, 508, 493, 547, 763, 497, 689, 625, 754, 676, 749, 683, 873, 571, 425, 697, 553, 762, 684, 757, 619, 809, 627, 417, 433, 369, 546, 692, 509, 825, 371, 690, 549, 441, 633, 700, 353, 865, 609, 377, 881, 361, 889),
    (772, 781, 795, 787, 789, 780, 771, 779, 529, 849, 530, 853, 532, 513, 841, 514, 517, 788, 729, 521, 601, 522, 603, 773, 796, 897, 537, 577, 538, 579, 797, 516, 705, 473, 475, 585, 593, 457, 597, 708, 713, 595, 721, 833, 845, 905, 715, 409, 641, 410, 857, 385, 657, 449, 913, 393, 665, 465, 921, 649, 401, 0, 0, 0, 0, 0, 0, 0, 0, 0),
    (805, 812, 821, 828, 545, 865, 813, 548, 569, 881, 829, 804, 737, 745, 889, 869, 820, 753, 609, 489, 490, 491, 573, 572, 481, 553, 873, 497, 498, 483, 885, 740, 561, 689, 505, 506, 441, 893, 748, 425, 427, 756, 625, 673, 697, 613, 417, 418, 433, 681, 633, 617, 761, 0, 0, 0, 0, 0, 0, 0, 0, 0, 0, 0, 0, 0, 0, 0, 0, 0),
    (853, 860, 845, 836, 601, 769, 897, 771, 605, 604, 577, 777, 905, 779, 581, 580, 593, 529, 641, 530, 597, 844, 521, 785, 913, 522, 787, 837, 772, 537, 793, 921, 538, 645, 532, 657, 513, 729, 585, 514, 661, 540, 473, 475, 649, 705, 665, 796, 721, 449, 451, 465, 466, 713, 457, 0, 0, 0, 0, 0, 0, 0, 0, 0, 0, 0, 0, 0, 0, 0),
    (869, 876, 885, 868, 609, 809, 929, 811, 893, 812, 625, 825, 937, 827, 613, 628, 633, 545, 689, 546, 877, 548, 561, 801, 697, 690, 803, 441, 693, 884, 761, 817, 673, 562, 699, 425, 677, 892, 819, 569, 681, 570, 427, 417, 685, 828, 945, 419, 553, 737, 497, 498, 745, 505, 753, 953, 617, 481, 433, 489, 0, 0, 0, 0, 0, 0, 0, 0, 0, 0),
    (900, 901, 909, 908, 961, 641, 857, 969, 859, 645, 860, 977, 649, 833, 835, 985, 917, 916, 585, 601, 586, 603, 729, 925, 604, 602, 593, 577, 578, 777, 733, 924, 779, 594, 449, 665, 841, 785, 652, 843, 473, 513, 769, 514, 451, 465, 469, 849, 836, 713, 529, 530, 787, 721, 771, 457, 705, 537, 538, 851, 657, 793, 521, 0, 0, 0, 0, 0, 0, 0),
    (933, 932, 941, 940, 689, 873, 693, 876, 697, 865, 701, 700, 737, 673, 809, 811, 677, 948, 801, 681, 625, 803, 685, 628, 817, 819, 489, 617, 545, 546, 949, 956, 561, 562, 497, 499, 501, 553, 881, 554, 676, 957, 745, 569, 889, 570, 684, 621, 753, 481, 609, 825, 633, 761, 505, 0, 0, 0, 0, 0, 0, 0, 0, 0, 0, 0, 0, 0, 0, 0),
    (965, 973, 981, 989, 729, 897, 732, 777, 779, 733, 705, 905, 900, 785, 708, 781, 713, 857, 859, 849, 716, 789, 721, 913, 851, 513, 514, 908, 853, 657, 601, 603, 602, 769, 860, 725, 665, 921, 771, 793, 529, 916, 661, 641, 649, 593, 594, 585, 668, 833, 924, 841, 521, 652, 577, 537, 0, 0, 0, 0, 0, 0, 0, 0, 0, 0, 0, 0, 0, 0),
    (737, 929, 740, 741, 801, 803, 745, 937, 805, 817, 819, 489, 492, 561, 873, 562, 875, 821, 809, 497, 500, 505, 697, 811, 506, 565, 825, 508, 617, 945, 827, 618, 749, 865, 481, 700, 753, 625, 867, 626, 757, 569, 620, 570, 553, 761, 953, 765, 881, 883, 545, 546, 673, 689, 889, 891, 681, 609, 610, 633, 0, 0, 0, 0, 0, 0, 0, 0, 0, 0),
)
STAGES = (7, 15, 25, 36)
SOLVE = tuple(range(39, 63, 3))


def choose(values, bits):
    if len(set(values)) == 1:
        return jnp.int32(values[0])
    half = len(values) // 2
    return jnp.where(bits[0], choose(values[half:], bits[1:]), choose(values[:half], bits[1:]))


def table_kernel(pos, res, psf, part, own, tiles, load_sem, tile_sem):
    unit = 8 * lax.axis_index("z") + 2 * lax.axis_index("y") + lax.axis_index("core")
    slab = res.shape[1]
    rows = own.shape[1] - 2 * PAD
    blocks = own.shape[0]
    half = blocks * LANES // 2
    assert (rows, half) == (64, 1024)
    own_copies = [
        pltpu.make_async_copy(psf.at[0, :, pl.ds(b * LANES, LANES)], own.at[b, pl.ds(PAD, rows)], load_sem.at[b])
        for b in range(blocks)
    ]
    for copy in own_copies:
        copy.start()

    def place(k):
        return pos[0, k] - unit * slab, pos[1, k]

    tile_copies = []
    for k in range(STEPS):
        row, col = place(k)
        row = pl.multiple_of(jnp.clip(row, 0, slab - 1) & ~7, 8)
        col = pl.multiple_of(col & ~127, LANES)
        copy = pltpu.make_async_copy(res.at[0, pl.ds(row, 8), pl.ds(col, LANES)], tiles.at[k], tile_sem.at[k])
        copy.start()
        tile_copies.append(copy)
    for b in range(blocks):
        own[b, :PAD, :] = jnp.zeros((PAD, LANES), F32)
        own[b, PAD + rows :, :] = jnp.zeros((PAD, LANES), F32)
    for copy in own_copies:
        copy.wait()

    wide = lax.broadcasted_iota(jnp.int32, (8, LANES), 1)
    deep = lax.broadcasted_iota(jnp.int32, (8, LANES), 0)

    def placed(tile, base):
        return jnp.where(wide == base + deep, jnp.sum(tile, axis=1, keepdims=True), 0.0)

    part[...] = jnp.zeros((8, LANES), F32)
    for k0 in range(0, STEPS, 8):
        peaks = [(pos[0, k0 + s] + half - unit * rows, pos[1, k0 + s] + half) for s in range(8)]

        def couple(j, carry):
            places = [(row - pos[0, j], col - pos[1, j]) for row, col in peaks]
            away = [lax.shift_right_logical(row, 6) | lax.shift_right_logical(col, 11) for row, col in places]

            @pl.when(functools.reduce(jnp.minimum, away) == 0)
            def _():
                tile = jnp.zeros((8, LANES), F32)
                for s, ((row, col), far) in enumerate(zip(places, away)):
                    found = own[(col >> 7) & 15, pl.ds(PAD + (row & 63) - s, 8), :]
                    tile = tile + jnp.where((wide == jnp.where(far == 0, col & 127, -1)) & (deep == s), found, 0.0)
                at = pl.ds(j >> 2, 1)
                part[at, :] = part[at, :] + jnp.sum(placed(tile, LANES // 4 * (j & 3) + k0), axis=0, keepdims=True)

            return carry

        lax.fori_loop(0, min(k0 + 7, STEPS - 1), couple, 0)
    for copy in tile_copies:
        copy.wait()
    last = STEPS // 4 - 1
    for k0 in range(0, STEPS, 8):
        places = [place(k0 + s) for s in range(8)]
        holds = [(row >= 0) & (row < slab) for row, _ in places]

        @pl.when(functools.reduce(jnp.logical_or, holds))
        def _():
            tile = jnp.zeros((8, LANES), F32)
            for s, ((row, col), held) in enumerate(zip(places, holds)):
                found = jnp.where((wide == (col & 127)) & (deep == jnp.where(held, row & 7, -1)), tiles[k0 + s], 0.0)
                tile = tile + jnp.where(deep == s, jnp.sum(found, axis=0, keepdims=True), 0.0)
            found = jnp.sum(placed(tile, LANES * 3 // 4 + k0), axis=0, keepdims=True)
            part[last : last + 1, :] = part[last : last + 1, :] + found


def peak_table(positions, residual, psf):
    rows, patch = psf.shape[1:]
    sems = pltpu.SemaphoreType.DMA
    return pl.pallas_call(
        table_kernel,
        out_shape=pltpu.VMEM((8, LANES), F32),
        in_specs=[pl.BlockSpec(memory_space=pltpu.SMEM)] + [pl.BlockSpec(memory_space=pltpu.HBM)] * 2,
        out_specs=pl.BlockSpec(memory_space=pltpu.VMEM),
        scratch_shapes=[pltpu.VMEM((patch // LANES, rows + 2 * PAD, LANES), F32), pltpu.VMEM((STEPS, 8, LANES), F32), sems((patch // LANES,)), sems((STEPS,))],
        compiler_params=pltpu.CompilerParams(vmem_limit_bytes=8 * 1024 * 1024),
        name="table",
    )(positions, pinned(residual, pltpu.HBM), pinned(psf, pltpu.HBM))


pinned = pltpu.with_memory_space_constraint


def gather_kernel(first_part, psf, res, g, amps, img, part, got, table, load_sem, send_sem, recv_sem, peer_send, peer_recv, sum_send, sum_recv):
    x, z, y, core = (lax.axis_index(a) for a in ("chan",) + ROWS)
    coord = {"z": z, "y": y, "chan": x, "core": core}
    size = {"z": 4, "y": 4, "chan": 4, "core": 2}
    rows = psf.shape[1]
    blocks = g.shape[0]
    count = blocks // PIECES

    def device(axis, step):
        return {axis: lax.rem(coord[axis] + step % size[axis], size[axis])}

    barrier = pltpu.get_barrier_semaphore()
    greeted = [("core", 1)] + [(axis, step) for axis in ("y", "z", "chan") for step in (1, 2, 3)]
    for axis, step in greeted:
        pl.semaphore_signal(barrier, inc=1, device_id=device(axis, step), device_id_type=MESH)

    chip = 4 * z + y
    unit = 2 * chip + core
    bits = [((unit >> n) & 1) == 1 for n in (4, 3, 2, 1, 0)]
    packed = [
        choose([sum(c << 10 * n for n, c in enumerate(p[t : t + 3])) for p in PROGRAM], bits) for t in range(0, len(PROGRAM[0]), 3)
    ]
    place_copies = [
        pltpu.make_async_copy(psf.at[0, :, pl.ds(b * LANES, LANES)], g.at[b, pl.ds(unit * rows, rows)], load_sem.at[b])
        for b in range(blocks)
    ]
    image_copy = pltpu.make_async_copy(res.at[0], img, load_sem.at[blocks])
    for copy in place_copies:
        copy.start()
    image_copy.start()
    for copy in place_copies:
        copy.wait()
    pl.semaphore_wait(barrier, len(greeted))

    def block(slot):
        return g.at[pl.ds((slot & 3) * count, count), pl.ds(pl.multiple_of((slot >> 2) * rows, rows), rows)]

    def remote(slot, sems, where):
        return pltpu.make_async_remote_copy(block(slot), block(slot), *sems, device_id=where, device_id_type=MESH)

    def share(slot):
        return remote(slot, (peer_send.at[slot], peer_recv.at[slot]), device("core", 1))

    def exchange(n):
        axis, steps, at = stages[n]
        return [
            pltpu.make_async_remote_copy(
                part.at[n] if n else first_part, got.at[at + m], sum_send.at[at + m], sum_recv.at[at + m], device_id=device(axis, step), device_id_type=MESH
            )
            for m, step in enumerate(steps)
        ]

    def spread():
        tables = [part[3]] + [got[7 + m] for m in range(3)]
        for i in range(STEPS // 4):
            rows_of = jnp.concatenate([t[i : i + 1, :] for t in tables] + [jnp.zeros((4, LANES), F32)], axis=0)
            for m in range(4):
                table[4 * i + m] = rows_of if m == 0 else pltpu.roll(rows_of, LANES - LANES // 4 * m, 1)

    wide = lax.broadcasted_iota(jnp.int32, (8, LANES), 1)

    def solve(j, left):
        value = jnp.sum(jnp.where(wide == j, left, 0.0), axis=1, keepdims=True)
        amp = 0.25 * (value + jnp.sum(value, axis=0, keepdims=True) / 4)
        amps[j] = jnp.broadcast_to(amp[0:1, :], (8, LANES))
        return left - amp * table[j]

    stages = [("core", (1,), 0), ("y", (1, 2, 3), 1), ("z", (1, 2, 3), 4), ("chan", (3, 2, 1), 7)]
    copies = exchange(0)
    for copy in copies:
        copy.start()
    for piece in range(PIECES):
        share(unit * PIECES + piece).start()
    sends = []
    for t in range(len(PROGRAM[0])):
        if t in STAGES:
            n = STAGES.index(t)
            for copy in copies:
                copy.wait()
            if n < 3:
                _, steps, at = stages[n]
                part[n + 1] = sum((got[at + m] for m in range(len(steps))), part[n] if n else first_part[...])
                copies = exchange(n + 1)
                for copy in copies:
                    copy.start()
            else:
                spread()
                left = table[STEPS - 1]
        if t in SOLVE:
            j = STEPS // len(SOLVE) * SOLVE.index(t)
            left = lax.fori_loop(j, j + STEPS // len(SOLVE), solve, left)
        code = packed[t // 3] >> 10 * (t % 3)
        kind, slot = code & 7, (code >> 3) & 127
        up = jnp.where(kind == 2, 1, jnp.where(kind == 3, 3, 0))
        over = jnp.where(kind == 4, 1, jnp.where(kind == 5, 3, 0))
        copy = remote(slot, (send_sem.at[t], recv_sem.at[slot]), {"z": (z + up) & 3, "y": (y + over) & 3})
        shard = slot >> 2
        mine = share(slot)
        if any(p[t] % 8 == 1 for p in PROGRAM):
            pl.when(kind == 1)(copy.wait_recv)
            pl.when((kind == 1) & (shard >= chip) & (shard <= chip + 16))(mine.start)
        if any(p[t] % 8 > 1 for p in PROGRAM):
            pl.when(kind > 1)(copy.start)
            sends.append((kind > 1, copy))
    image_copy.wait()
    for n in range(9):
        for piece in range(PIECES):
            theirs = chip + ((chip + 1 - core) & 1) + 2 * n
            ours = chip + ((chip + core) & 1) + 2 * n
            pl.when(theirs <= chip + 16)(share(theirs * PIECES + piece).wait_recv)
            pl.when(ours <= chip + 16)(share(ours * PIECES + piece).wait_send)
    for sent, copy in sends:
        pl.when(sent)(copy.wait_send)


def gather(part, psf, residual):
    patch = psf.shape[2]
    blocks = patch // LANES
    sems = pltpu.SemaphoreType.DMA
    return pl.pallas_call(
        gather_kernel,
        out_shape=(pltpu.VMEM((blocks, patch, LANES), F32), pltpu.VMEM((STEPS, 8, LANES), F32), pltpu.VMEM(residual.shape[1:], F32)),
        in_specs=[pl.BlockSpec(memory_space=pltpu.VMEM)] + [pl.BlockSpec(memory_space=pltpu.HBM)] * 2,
        out_specs=(pl.BlockSpec(memory_space=pltpu.VMEM),) * 3,
        scratch_shapes=[
            pltpu.VMEM((4, 8, LANES), F32),
            pltpu.VMEM((10, 8, LANES), F32),
            pltpu.VMEM((STEPS, 8, LANES), F32),
            sems((blocks + 1,)),
            sems((len(PROGRAM[0]),)),
            sems((32 * PIECES,)),
            sems((32 * PIECES,)),
            sems((32 * PIECES,)),
            sems((10,)),
            sems((10,)),
        ],
        compiler_params=pltpu.CompilerParams(collective_id=0, has_side_effects=True, vmem_limit_bytes=8 * 1024 * 1024),
        name="gather",
    )(pinned(part, pltpu.VMEM), pinned(psf, pltpu.HBM), pinned(residual, pltpu.HBM))


def apply_kernel(pos, amps, g, given, img):
    slab, ncols = img.shape
    blocks = g.shape[0]
    half = blocks * LANES // 2
    first = slab * (8 * lax.axis_index("z") + 2 * lax.axis_index("y") + lax.axis_index("core"))
    lane = lax.broadcasted_iota(jnp.int32, (8, LANES), 1)
    groups = slab // 8

    def step(k, carry):
        start = first - pos[0, k] + half
        left = pos[1, k] - half
        block, shift = left >> 7, left & 127
        tail = lane >= shift
        amp = amps[k]
        before = [jnp.zeros((8, LANES), F32)] * groups

        def columns(j):
            col = jnp.minimum(block + j, ncols // LANES - 1) if j == blocks else block + j
            return pl.ds(pl.multiple_of(col * LANES, LANES), LANES)

        def subtract(terms):
            old = [[img[8 * i : 8 * i + 8, columns(j)] for i in range(groups)] for j, _ in terms]
            for (j, term), o in zip(terms, old):
                for i in range(groups):
                    img[8 * i : 8 * i + 8, columns(j)] = o[i] - term[i]

        pending = []
        for js in [range(j, j + 4) for j in range(0, blocks, 4)] + [[blocks]]:
            terms = []
            for j in js:
                if j < blocks:
                    now = [pltpu.roll(g[j, pl.ds(start + 8 * i, 8), :] * amp, shift, 1) for i in range(groups)]
                else:
                    now = [jnp.zeros((8, LANES), F32)] * groups
                terms.append((j, [jnp.where(tail, n, b) for n, b in zip(now, before)]))
                before = now
            subtract(pending)
            pending = terms
        subtract(pending)
        return carry

    lax.fori_loop(0, STEPS, step, 0, unroll=4)


def apply_steps(positions, amps, g, image):
    return pl.pallas_call(
        apply_kernel,
        out_shape=pltpu.VMEM(image.shape, F32),
        in_specs=[pl.BlockSpec(memory_space=pltpu.SMEM)] + [pl.BlockSpec(memory_space=pltpu.VMEM)] * 3,
        out_specs=pl.BlockSpec(memory_space=pltpu.VMEM),
        input_output_aliases={3: 0},
        compiler_params=pltpu.CompilerParams(vmem_limit_bytes=8 * 1024 * 1024),
        name="apply",
    )(positions, *(pinned(a, pltpu.VMEM) for a in (amps, g, image)))


SPLIT = 4


def reduce_kernel(img, parts, scale, far, near, sums, squares, got, far_send, far_recv, near_send, near_recv, sums_send, sums_recv, sq_send, sq_recv):
    x, z, y, core = (lax.axis_index(a) for a in ("chan",) + ROWS)
    half, width = img.shape[0] // 2, parts.shape[1]
    piece = width // SPLIT

    close = [(dx, dc) for dc in range(2) for dx in range(4) if (dx, dc) != (0, 0)]
    plane = [(dz, dy) for dz in range(4) for dy in range(4) if (dz, dy) != (0, 0)]

    def near_id(dx, dc):
        return {"chan": (x + dx) & 3, "core": (core + dc) & 1}

    def plane_id(dz, dy):
        return {"z": (z + dz) & 3, "y": (y + dy) & 3}

    peers = [near_id(*d) for d in close] + [plane_id(*d) for d in plane]
    barrier = pltpu.get_barrier_semaphore()
    for peer in peers:
        pl.semaphore_signal(barrier, inc=1, device_id=peer, device_id_type=MESH)
    pl.semaphore_wait(barrier, len(peers))

    def cols(chunk, q):
        return pl.ds(pl.multiple_of(((x + chunk) & 3) * width + q * piece, piece), piece)

    def rows(which):
        return pl.ds(which * half, half)

    def send(src, dst, n, q, sems, way):
        copy = pltpu.make_async_remote_copy(
            src, dst.at[n, :, pl.ds(q * piece, piece)], sems[0].at[n * SPLIT + q], sems[1].at[n * SPLIT + q],
            device_id={"chan": (x + way) & 3}, device_id_type=MESH,
        )
        copy.start()
        return copy

    ways = (1, -1)
    fars, nears, lasts = {}, {}, {}
    for q in range(SPLIT):
        for n, way in enumerate(ways):
            fars[n, q] = send(img.at[rows(1 - n), cols(2, q)], far, n, q, (far_send, far_recv), way)
    for q in range(SPLIT):
        for n, way in enumerate(ways):
            nears[n, q] = send(img.at[rows(n), cols(way, q)], near, n, q, (near_send, near_recv), way)
    for q in range(SPLIT):
        for n, way in enumerate(ways):
            fars[n, q].wait_recv()
            at = pl.ds(q * piece, piece)
            far[n, :, at] = far[n, :, at] + img[rows(1 - n), cols(way, q)]
            lasts[n, q] = send(far.at[n, :, at], sums, n, q, (sums_send, sums_recv), way)
    total = jnp.zeros((8, LANES), F32)
    for q in range(SPLIT):
        at = pl.ds(q * piece, piece)
        for n in range(2):
            nears[n, q].wait_recv()
            parts[rows(n), at] = img[rows(n), cols(0, q)] + near[n, :, at]
    for q in range(SPLIT):
        at = pl.ds(q * piece, piece)
        for n in range(2):
            lasts[n, q].wait_recv()
            value = parts[rows(1 - n), at] + sums[n, :, at]
            parts[rows(1 - n), at] = value
            square = value * value
            for i in range(half // 8):
                for t in range(piece // LANES):
                    total = total + square[8 * i : 8 * i + 8, LANES * t : LANES * (t + 1)]

    squares[0] = total
    done = []
    for stage, ids, start in ((0, peers[: len(close)], 0), (1, peers[len(close) :], len(close))):
        copies = [
            pltpu.make_async_remote_copy(squares.at[stage], got.at[start + i], sq_send.at[start + i], sq_recv.at[start + i], device_id=peer, device_id_type=MESH)
            for i, peer in enumerate(ids)
        ]
        for copy in copies:
            copy.start()
        for copy in copies:
            copy.wait_recv()
        done += copies
        squares[stage + 1] = sum((got[start + i] for i in range(len(ids))), squares[stage])
    total = jnp.sum(jnp.sum(squares[2], axis=1, keepdims=True), axis=0, keepdims=True)
    count = img.shape[0] * img.shape[1] * 32
    scale[...] = jnp.broadcast_to(lax.rsqrt(total / count + 1e-06), (8, LANES))
    for copy in list(fars.values()) + list(nears.values()) + list(lasts.values()) + done:
        copy.wait_send()


def reduce_channels(image):
    slab, ncols = image.shape
    width = ncols // 4
    sems = pltpu.SemaphoreType.DMA
    return pl.pallas_call(
        reduce_kernel,
        out_shape=(pltpu.VMEM((slab, width), F32), pltpu.VMEM((8, LANES), F32)),
        in_specs=[pl.BlockSpec(memory_space=pltpu.VMEM)],
        out_specs=(pl.BlockSpec(memory_space=pltpu.VMEM),) * 2,
        scratch_shapes=[pltpu.VMEM((2, slab // 2, width), F32)] * 3
        + [pltpu.VMEM((3, 8, LANES), F32), pltpu.VMEM((22, 8, LANES), F32)]
        + [sems((2 * SPLIT,))] * 6
        + [sems((22,))] * 2,
        compiler_params=pltpu.CompilerParams(collective_id=1, has_side_effects=True, vmem_limit_bytes=8 * 1024 * 1024),
        name="reduce",
    )(pinned(image, pltpu.VMEM))


def write_kernel(img, parts, scale, image_out, normal_out, normal, sems):
    copies = [pltpu.make_async_copy(img, image_out.at[0], sems.at[0])]
    copies[0].start()
    piece = parts.shape[1] // 4
    for q in range(4):
        at = pl.ds(q * piece, piece)
        normal[:, at] = parts[:, at] * scale[0:1, 0:1]
        copies.append(pltpu.make_async_copy(normal.at[:, at], normal_out.at[:, at], sems.at[q + 1]))
        copies[-1].start()
    for copy in copies:
        copy.wait()


def write(image, parts, scale):
    return pl.pallas_call(
        write_kernel,
        out_shape=(pltpu.HBM((1,) + image.shape, F32), pltpu.HBM(parts.shape, F32)),
        in_specs=[pl.BlockSpec(memory_space=pltpu.VMEM)] * 3,
        out_specs=(pl.BlockSpec(memory_space=pltpu.HBM),) * 2,
        scratch_shapes=[pltpu.VMEM(parts.shape, F32), pltpu.SemaphoreType.DMA((5,))],
        compiler_params=pltpu.CompilerParams(vmem_limit_bytes=8 * 1024 * 1024),
        name="write",
    )(*(pinned(a, pltpu.VMEM) for a in (image, parts, scale)))


def on_device(residual, psf, positions):
    positions = positions.T
    part = peak_table(positions, residual, psf)
    g, amps, image = gather(part, psf, residual)
    image = apply_steps(positions, amps, g, image)
    parts, scale = reduce_channels(image)
    return write(image, parts, scale)


def solution(mesh):
    finer = Mesh(mesh.devices.reshape(mesh.shape["chan"], 4, 4, 2), ("chan",) + ROWS)
    return jax.shard_map(
        on_device,
        mesh=finer,
        in_specs=(P("chan", ROWS, None), P("chan", ROWS, None), P()),
        out_specs=(P("chan", ROWS, None), P(ROWS, "chan")),
        check_vma=False,
    )
```
